32 devices in a mesh: blk: 16 (over z, y, x), grp: 2 (over core).
Axes of the slice: x: 2, y: 2, z: 4, core: 2. Of those that a mesh axis runs over, the one named last changes fastest.
Arguments:
- returns: float32 [512, 8192], P(None, ('blk', 'grp')), may hold values from -200 to 200
Outputs:
- correlation: bfloat16 [8192, 8192], P(('blk', 'grp'))
The draws below stay inside these ranges and needn't reach their ends.
All inputs are finite; a program needn't handle non-finite values.
Results may differ from the reference program's by a relative error of at most 0.0034.
Values may be sent and summed in bfloat16 or wider, within the bound.
A program may use at most 128 MiB of HBM per device.

```python
import math
import jax
import jax.numpy as jnp
from jax import lax

SER_DEV = 256
BARS = 512
SERIES = 8192


def draw_returns(key, part):
    subkeys = jax.random.split(key, 4)
    factor = jnp.clip(jax.random.normal(subkeys[0], (BARS, 1), jnp.float32), -4.0, 4.0)
    position = jnp.arange(SERIES, dtype=jnp.float32)[None, :] / SERIES
    loading = 0.5 + position + 0.3 * jnp.clip(jax.random.normal(subkeys[1], (1, SERIES), jnp.float32), -4.0, 4.0)
    volatility = jnp.exp(jax.random.uniform(subkeys[2], (1, SERIES), jnp.float32, math.log(0.3), math.log(3.0)))
    specific = 0.7 * jnp.clip(jax.random.normal(subkeys[3], (BARS, SERIES), jnp.float32), -4.0, 4.0)
    return (volatility * (factor * loading + specific)).astype(jnp.float32)


def setup_inputs(seed: int = 0) -> dict:
    arg_keys = jax.random.split(jax.random.key(seed), 2)
    returns = draw_returns(jax.random.fold_in(arg_keys[1], 71), 0)
    return {"returns": returns}


def reference(returns):
    market = lax.optimization_barrier(jnp.mean(returns, axis=1, keepdims=True))
    excess = returns - market
    deviation = excess - lax.optimization_barrier(jnp.mean(excess, axis=0, keepdims=True))
    inverse = lax.rsqrt(lax.optimization_barrier(jnp.mean(deviation * deviation, axis=0, keepdims=True)) + 1e-06) / math.sqrt(BARS)
    zscores = (deviation * inverse).astype(jnp.bfloat16)
    blocks = SERIES // SER_DEV
    columns = jnp.arange(SERIES, dtype=jnp.int32) // SER_DEV

    def row_block(row_index):
        block_rows = lax.dynamic_slice_in_dim(zscores, (row_index * SER_DEV).astype(jnp.int32), SER_DEV, 1)
        products = lax.dot_general(block_rows, zscores, (((0,), (0,)), ((), ())), preferred_element_type=jnp.float32)
        return jnp.where(columns[None, :] >= row_index, products, jnp.float32(0.0)).astype(jnp.bfloat16)
    stacked = lax.map(row_block, jnp.arange(blocks, dtype=jnp.int32))
    return stacked.reshape(SERIES, SERIES)
```

```python
import functools
import math

import jax
import jax.numpy as jnp
from jax import lax
from jax.experimental import pallas as pl
from jax.experimental.pallas import tpu as pltpu
from jax.sharding import PartitionSpec as P

MESH = pl.DeviceIdType.MESH
DOWN = ("ZA", "ZB", "ZO", "ZX", "ZY", "ZD")
SPREAD = ("XA", "XB", "YA", "YB", "D0", "D1")
REST = ("XR", "YR")
PARTNER = ("P0", "P1", "P2", "P3", "P4")
KINDS = DOWN + SPREAD + REST + PARTNER
WAITS = {
    "ZA": -0.99, "ZB": -0.69, "ZO": 1.78, "ZX": 1.11, "ZY": 0.89, "ZD": 2.22, "XA": 0.73, "XB": 1.51,
    "YA": 1.22, "YB": 0.52, "XR": 1.64, "YR": 0.76, "D0": 2.25, "D1": 2.77, "M0": 2.85, "M1": 3.16,
}
SENDS = (
    "D1", "XA", "ZA", "P3", "P4", "ZD", "YB", "XR", "ZB", "ZX", "D0", "ZY", "P0", "ZO", "YR", "P2", "YA", "P1", "XB",
)


def needs(kind, d):
    first = d == 0
    return {
        "ZA": [] if first else ["ZA"],
        "ZB": [] if first else ["ZB"],
        "ZO": [] if first else ["ZO"],
        "ZX": ["XR"] if first else ["ZX"],
        "ZY": ["YR"] if first else ["ZY"],
        "ZD": ["D1"] if first else ["ZD"],
        "XA": [] if first else ["ZA"],
        "YA": [] if first else ["ZA"],
        "XB": [] if first else ["ZB"],
        "YB": [] if first else ["ZB"],
        "XR": [],
        "YR": [],
        "D0": ["XA"],
        "D1": ["YB", "YR"] if first else ["YB"],
        "P0": [] if first else ["ZA", "ZB", "ZO"],
        "P1": ["XA", "XB", "XR" if first else "ZX"],
        "P2": ["YA", "YB", "YR" if first else "ZY"],
        "P3": ["D0"],
        "P4": ["D1"] if first else ["D1", "ZD"],
    }[kind]


def sends_down(action, kind, d):
    return kind in DOWN and action in ("start", "drain")


def plan(planes):
    events = []
    for d in range(planes):
        kinds = SPREAD + (DOWN if d else REST) + ("M0", "M1")
        events += [(d + WAITS[kind], kind, d) for kind in kinds]
    here, sent, actions = set(), set(), []

    def send():
        for d in range(planes):
            for kind in SENDS:
                absent = (kind in REST and d > 0) or (kind in DOWN and d == planes - 1)
                if (kind, d) not in sent and not absent and all((k, d) in here for k in needs(kind, d)):
                    sent.add((kind, d))
                    actions.append(("start", kind, d))

    send()
    for _, kind, d in sorted(events):
        if kind in ("M0", "M1"):
            actions.extend(("wait", k, d) for k in (PARTNER[:3] if kind == "M0" else PARTNER[3:]))
            actions.append(("multiply", kind, d))
        else:
            actions.append(("wait", kind, d))
            here.add((kind, d))
            send()
    return actions


def kernel(planes, r_hbm, out_ref, r_ref, gath, zt, parts, load_sem, psend, precv, send, recv):
    bars, width = r_ref.shape
    series = width * gath.shape[0]
    blk, core = lax.axis_index("blk"), lax.axis_index("grp")
    x, y, z = lax.rem(blk, 2), lax.rem(lax.div(blk, 2), 2), lax.div(blk, 4)
    nx, ny, nc = 1 - x, 1 - y, 1 - core

    def device(zz, yy, xx, cc):
        return {"blk": (zz * 2 + yy) * 2 + xx, "grp": cc}

    def slot(zz, yy, xx, cc):
        return ((zz * 2 + yy) * 2 + xx) * 2 + cc

    load = pltpu.make_async_copy(r_hbm, r_ref, load_sem)
    load.start()
    others = [
        ((z + d) % planes, ny if j & 2 else y, nx if j & 1 else x, nc if j & 4 else core)
        for d in [*range(1, planes), 0]
        for j in range(8)
        if d or j
    ]
    barrier = pltpu.get_barrier_semaphore()
    for other in others:
        pl.semaphore_signal(barrier, inc=1, device_id=device(*other), device_id_type=MESH)
    load.wait()

    lanes = r_ref[:, :128]
    for i in range(1, width // 128):
        lanes = lanes + r_ref[:, 128 * i : 128 * (i + 1)]
    own = slot(z, y, x, core)
    parts[own] = jnp.sum(lanes.T, axis=0, keepdims=True)
    pl.semaphore_wait(barrier, len(others))
    part_copies = [
        pltpu.make_async_remote_copy(
            parts.at[own], parts.at[own], psend, precv, device_id=device(*other), device_id_type=MESH
        )
        for other in others
    ]
    for part in part_copies:
        part.start()
    rest = parts.at[pl.ds(0, len(others))]
    all_parts = pltpu.make_async_remote_copy(
        rest, rest, psend, precv, device_id=device(*others[0]), device_id_type=MESH
    )
    all_parts.wait_recv()
    market = jnp.sum(parts[...], axis=0) * (1.0 / series)
    market = jnp.broadcast_to(market, (128, bars)).T
    for i in range(width // 128):
        excess = r_ref[:, 128 * i : 128 * (i + 1)] - market
        deviation = excess - jnp.mean(excess, axis=0, keepdims=True)
        inverse = lax.rsqrt(jnp.mean(deviation * deviation, axis=0, keepdims=True) + 1e-06) / math.sqrt(bars)
        gath[own, :, 128 * i : 128 * (i + 1)] = (deviation * inverse).astype(jnp.bfloat16)

    high = bars * 25 // 32 // 16 * 16
    half = bars * 13 // 32 // 16 * 16
    rows_a, rows_b, rows_r = (0, half), (half, high - half), (high, bars - high)

    def copy(kind, d, arriving):
        zz = z + d
        link = kind[0] if kind[0] != "D" else ("Y" if kind == "D0" else "X")
        down = link == "Z"
        if arriving:
            flip = {"X": (0, 1), "Y": (1, 0), "D": (1, 1)}.get(kind[0], (0, 0))
        else:
            flip = {"D0": (0, 1), "D1": (1, 0)}.get(kind, (0, 0))
        if down:
            flip = {"ZX": (0, 1), "ZY": (1, 0), "ZD": (1, 1)}.get(kind, (0, 0))
            rows = {"ZA": rows_a, "ZB": rows_b}.get(kind, rows_r)
        elif link == "P":
            flip = {"P0": (0, 0), "P1": (0, 1), "P2": (1, 0)}.get(kind, (1, 1))
            rows = {"P3": rows_a, "P4": (half, bars - half)}.get(kind, (0, bars))
        else:
            last = (half, bars - half) if d == 0 else rows_b
            rows = {"A": rows_a, "B": rows_b, "R": rows_r, "0": rows_a, "1": last}[kind[1]]
        owner = nc if link == "P" and arriving else core
        block = slot(zz, ny if flip[0] else y, nx if flip[1] else x, owner)
        target = {
            "Z": device(z - 1, y, x, core),
            "X": device(z, y, nx, core),
            "Y": device(z, ny, x, core),
            "P": device(z, y, x, nc),
        }[link]
        ref, k = gath.at[block, pl.ds(*rows)], KINDS.index(kind)
        return pltpu.make_async_remote_copy(
            ref,
            ref,
            send.at[k, d],
            recv.at[k, d + 1 if down and not arriving else d],
            device_id=target,
            device_id_type=MESH,
        )

    def multiply(kind, d):
        base, count = (0, 6) if kind == "M0" else (6, 2)

        @pl.loop(0, count)
        def _(i):
            chip, other = lax.div(i + base, 2), lax.rem(i, 2)
            flip_x, flip_y = lax.rem(chip, 2), lax.div(chip, 2)
            block = slot(z + d, y + flip_y * (1 - 2 * y), x + flip_x * (1 - 2 * x), other)
            at = pl.ds(pl.multiple_of(block * width, width), width)
            out_ref[:, at] = jnp.dot(zt[...], gath[block], preferred_element_type=jnp.float32).astype(jnp.bfloat16)

    def act(action, kind, d):
        if action == "multiply":
            multiply(kind, d)
        elif action == "wait":
            copy(kind, d, True).wait_recv()
        else:
            end = copy(kind, d, False)
            (end.start if action == "start" else end.wait_send)()

    actions = plan(planes)
    actions += [("drain", kind, d) for action, kind, d in actions if action == "start"]
    transposed = False
    while actions:
        key = (actions[0][2], sends_down(*actions[0]))
        count = 1
        while count < len(actions) and (actions[count][2], sends_down(*actions[count])) == key:
            count += 1
        batch, actions = actions[:count], actions[count:]

        def run(batch=batch):
            for action in batch:
                act(*action)

        if not transposed and batch[0][0] != "start":
            zt[...] = gath[own].T
            transposed = True
        d, down = key
        if down:
            pl.when(jnp.minimum(z, planes - z - d) > 0)(run)
        elif d:
            pl.when(z + d < planes)(run)
        else:
            run()
    all_parts.wait_send()


def shards(planes, returns):
    bars, width = returns.shape
    blocks = planes * 8
    held = blocks * width * (2 * bars + 2 * width) + 6 * bars * width
    products = pl.pallas_call(
        functools.partial(kernel, planes),
        out_shape=jax.ShapeDtypeStruct((width, blocks * width), jnp.bfloat16),
        in_specs=[pl.BlockSpec(memory_space=pltpu.HBM)],
        out_specs=pl.BlockSpec(memory_space=pltpu.VMEM),
        scratch_shapes=[
            pltpu.VMEM((bars, width), jnp.float32),
            pltpu.VMEM((blocks, bars, width), jnp.bfloat16),
            pltpu.VMEM((width, bars), jnp.bfloat16),
            pltpu.VMEM((blocks, 1, bars), jnp.float32),
            pltpu.SemaphoreType.DMA,
            pltpu.SemaphoreType.DMA,
            pltpu.SemaphoreType.DMA,
            pltpu.SemaphoreType.DMA((len(KINDS), planes)),
            pltpu.SemaphoreType.DMA((len(KINDS), planes)),
        ],
        compiler_params=pltpu.CompilerParams(
            collective_id=0, has_side_effects=True, vmem_limit_bytes=held + 4 * 1024 * 1024
        ),
    )(pltpu.with_memory_space_constraint(returns, pltpu.HBM))
    my_index = lax.axis_index(("blk", "grp"))
    column_block = jnp.arange(blocks * width, dtype=jnp.int32) // width
    return jnp.where(column_block[None, :] >= my_index, products, jnp.bfloat16(0.0))


def solution(mesh):
    planes = mesh.shape["blk"] // 4
    in_specs = (P(None, ("blk", "grp")),)
    out_specs = P(("blk", "grp"), None)
    return jax.shard_map(
        functools.partial(shards, planes), mesh=mesh, in_specs=in_specs, out_specs=out_specs, check_vma=False
    )
```

```python
import functools
import math

import jax
import jax.numpy as jnp
from jax import lax
from jax.experimental import pallas as pl
from jax.experimental.pallas import tpu as pltpu
from jax.sharding import PartitionSpec as P

MESH = pl.DeviceIdType.MESH
DOWN = ("ZA", "ZB", "ZO", "ZX", "ZY", "ZD")
SPREAD = ("XA", "XB", "YA", "YB", "D0", "D1")
REST = ("XR", "YR")
PARTNER = ("P0", "P1", "P2", "P3", "P4")
KINDS = DOWN + SPREAD + REST
WAITS = (
    {
        "XA": 0, "XB": 2, "XR": 4, "YR": 5, "YA": 6, "YB": 7, "D0": 8, "M0": 12,
        "D1": 18, "M1": 41,
    },
    {
        "ZA": 1, "ZB": 3, "XA": 9, "YA": 11, "XB": 14, "ZX": 15, "YB": 16, "ZY": 17,
        "D0": 21, "ZO": 23, "ZD": 28, "D1": 32, "M1": 38, "M0": 45,
    },
    {
        "ZA": 10, "ZB": 13, "XA": 22, "ZY": 24, "YB": 25, "ZX": 26, "XB": 27, "YA": 30,
        "ZO": 31, "M0": 35, "ZD": 39, "D1": 40, "D0": 42, "M1": 49,
    },
    {
        "ZA": 19, "ZB": 20, "XA": 29, "YB": 33, "YA": 34, "XB": 36, "ZY": 37, "ZX": 43,
        "ZO": 44, "D0": 46, "ZD": 47, "D1": 48, "M0": 50, "M1": 51,
    },
)
PERIOD = 16
STATS = (("XA", 0), ("YA", 0), ("ZA", 1))
SENDS = (
    "XB", "D1", "YA", "ZD", "ZA", "XA", "P0", "ZY", "ZB", "P2", "YR", "D0", "P3", "P1", "YB", "ZX", "ZO", "XR", "P4",
)


def needs(kind, d):
    first = d == 0
    return {
        "ZA": [] if first else ["ZA"],
        "ZB": [] if first else ["ZB"],
        "ZO": [] if first else ["ZO"],
        "ZX": ["XR"] if first else ["ZX"],
        "ZY": ["YR"] if first else ["ZY"],
        "ZD": ["D1"] if first else ["ZD"],
        "XA": [] if first else ["ZA"],
        "YA": [] if first else ["ZA"],
        "XB": [] if first else ["ZB"],
        "YB": [] if first else ["ZB"],
        "XR": [],
        "YR": [],
        "D0": ["XA"],
        "D1": ["YB", "YR"] if first else ["YB"],
        "P0": [] if first else ["ZA", "ZB", "ZO"],
        "P1": ["XA", "XB", "XR" if first else "ZX"],
        "P2": ["YA", "YB", "YR" if first else "ZY"],
        "P3": ["D0"],
        "P4": ["D1"] if first else ["D1", "ZD"],
    }[kind]


def group(action, kind, d):
    if action == "start" and kind in DOWN:
        return ("sends down", d)
    return ("holds", d)


def plan(planes):
    events = []
    for d in range(planes):
        kinds = SPREAD + (DOWN if d else REST) + ("M0", "M1")
        known = min(d, len(WAITS) - 1)
        events += [(WAITS[known][kind] + PERIOD * (d - known), kind, d) for kind in kinds]
    here, sent, actions = set(), set(), []

    def send():
        for d in range(planes):
            for kind in SENDS:
                absent = (kind in REST and d > 0) or (kind in DOWN and d == planes - 1)
                if (kind, d) not in sent and not absent and all((k, d) in here for k in needs(kind, d)):
                    sent.add((kind, d))
                    actions.append(("start", kind, d))

    for kind in ("XA", "YA", "ZA"):
        sent.add((kind, 0))
        actions.append(("start", kind, 0))
    send()
    for _, kind, d in sorted(events):
        if kind in ("M0", "M1"):
            actions.append(("wait", "P" + kind[1], d))
            actions.append(("multiply", kind, d))
        else:
            actions.append(("wait", kind, d))
            here.add((kind, d))
            send()
    return actions


def kernel(
    planes, r_hbm, out_ref, r_ref, gath, zt, parts, total, market, raw, stats, load_sem, psend, precv, send, recv
):
    bars, width = r_ref.shape
    blocks = gath.shape[0]
    low = min(2, planes)
    blk, core = lax.axis_index("blk"), lax.axis_index("grp")
    x, y, z = lax.rem(blk, 2), lax.rem(lax.div(blk, 2), 2), lax.div(blk, 4)
    nx, ny, nc = 1 - x, 1 - y, 1 - core
    high = bars * 26 // 32 // 16 * 16
    half = bars * 13 // 32 // 16 * 16
    rows_a, rows_b, rows_r = (0, half), (half, high - half), (high, bars - high)

    def device(zz, yy, xx, cc):
        return {"blk": (zz * 2 + yy) * 2 + xx, "grp": cc}

    def slot(zz, yy, xx, cc):
        return ((zz * 2 + yy) * 2 + xx) * 2 + cc

    own = slot(z, y, x, core)
    load = pltpu.make_async_copy(r_hbm, r_ref, load_sem)
    load.start()
    barrier = pltpu.get_barrier_semaphore()

    def greet(target):
        pl.semaphore_signal(barrier, inc=1, device_id=target, device_id_type=MESH)

    @pl.when(z < low)
    def _():
        for j in range(blocks):
            pl.when(own != j)(functools.partial(greet, {"blk": j // 2, "grp": j % 2}))

    @pl.when(z >= low)
    def _():
        for j in range(1, 8):
            greet(device(z, ny if j & 2 else y, nx if j & 1 else x, nc if j & 4 else core))
        pl.when(z < planes - 1)(lambda: greet(device(z + 1, y, x, core)))

    load.wait()
    lanes = r_ref[:, :128]
    for i in range(1, width // 128):
        lanes = lanes + r_ref[:, 128 * i : 128 * (i + 1)]
    parts[own] = jnp.sum(lanes.T, axis=0, keepdims=True)

    def part_copy(target):
        return pltpu.make_async_remote_copy(
            parts.at[own], parts.at[own], psend.at[0], precv.at[0], device_id=target, device_id_type=MESH
        )

    def part_wait(count):
        rest = parts.at[pl.ds(0, count)]
        return pltpu.make_async_remote_copy(
            rest, rest, psend.at[0], precv.at[0], device_id=device(z, y, x, nc), device_id_type=MESH
        )

    def total_copy(zz):
        return pltpu.make_async_remote_copy(
            total, total, psend.at[1], precv.at[1], device_id=device(zz, y, x, core), device_id_type=MESH
        )

    below = jnp.where(z < low, 8 * low - 1, 8 * low + 7 + jnp.where(z > low, 1, 0))
    pl.semaphore_wait(barrier, below)
    for j in range(8 * low):
        pl.when(own != j)(lambda j=j: part_copy({"blk": j // 2, "grp": j % 2}).start())

    recvs = {}
    for d in range(planes):
        for kind in SPREAD + (DOWN if d else REST) + ("P0", "P1"):
            recvs[kind, d] = len(recvs)

    def early(k, source, rows):
        kind, d, target = (
            ("XA", 0, device(z, y, nx, core)),
            ("YA", 0, device(z, ny, x, core)),
            ("ZA", 1, device(z - 1, y, x, core)),
        )[k]
        return pltpu.make_async_remote_copy(
            source,
            raw.at[k, pl.ds(*rows)],
            send.at[2 * planes + 2 + k // 2],
            recv.at[recvs[kind, d]],
            device_id=target,
            device_id_type=MESH,
        )

    raw_rows, stat_rows = (0, half), (half, 8)
    raw_source = r_ref.at[pl.ds(*raw_rows)]

    @pl.when(z < low)
    def _():
        early(0, raw_source, raw_rows).start()
        early(1, raw_source, raw_rows).start()

    if planes > 1:
        pl.when(z == 1)(lambda: early(2, raw_source, raw_rows).start())

    @pl.loop(0, z * 8)
    def _(block):
        at = pl.ds(pl.multiple_of(block * width, width), width)
        out_ref[:, at] = jnp.zeros((width, width), jnp.bfloat16)

    @pl.when(z < low)
    def _():
        part_wait(blocks - 1).wait_recv()
        total[...] = jnp.sum(parts[...], axis=0) * (1.0 / (width * blocks))

    if planes > low:

        @pl.when(z == low - 1)
        def _():
            for zz in range(low, planes):
                total_copy(zz).start()

        pl.when(z >= low)(lambda: total_copy(z).wait_recv())

    market[...] = jnp.broadcast_to(total[...], (128, bars)).T
    first = lax.broadcasted_iota(jnp.int32, (8, 128), 0) == 0
    for i in range(width // 128):
        at = slice(128 * i, 128 * (i + 1))
        excess = r_ref[:, at] - market[...]
        mean = jnp.mean(excess, axis=0, keepdims=True)
        deviation = excess - mean
        inverse = lax.rsqrt(jnp.mean(deviation * deviation, axis=0, keepdims=True) + 1e-06) / math.sqrt(bars)
        stats[:, at] = jnp.where(first, mean, inverse)
        gath[own, :, at] = (deviation * inverse).astype(jnp.bfloat16)

    def convert(k, block):
        early(k, raw.at[k], (0, half + 8)).wait_recv()
        for i in range(width // 128):
            at = slice(128 * i, 128 * (i + 1))
            deviation = raw[k, :half, at] - market[:half] - raw[k, half : half + 1, at]
            gath[block, :half, at] = (deviation * raw[k, half + 1 : half + 2, at]).astype(jnp.bfloat16)

    def piece(kind, d, arriving):
        link = kind[0] if kind[0] != "D" else ("Y" if kind == "D0" else "X")
        if arriving:
            flip = {"X": (0, 1), "Y": (1, 0), "D": (1, 1)}.get(kind[0], (0, 0))
        else:
            flip = {"D0": (0, 1), "D1": (1, 0)}.get(kind, (0, 0))
        if link == "Z":
            flip = {"ZX": (0, 1), "ZY": (1, 0), "ZD": (1, 1)}.get(kind, (0, 0))
            rows = {"ZA": rows_a, "ZB": rows_b}.get(kind, rows_r)
        elif link == "P":
            flip = {"P0": (0, 0), "P1": (0, 1), "P2": (1, 0)}.get(kind, (1, 1))
            rows = {"P3": rows_a, "P4": (half, bars - half)}.get(kind, (0, bars))
        else:
            last = (half, bars - half) if d == 0 else rows_b
            rows = {"A": rows_a, "B": rows_b, "R": rows_r, "0": rows_a, "1": last}[kind[1]]
        return link, flip, rows

    def copy(kind, d, arriving):
        link, flip, rows = piece(kind, d, arriving)
        down = link == "Z"
        block = slot(z + d, ny if flip[0] else y, nx if flip[1] else x, core)
        target = {
            "Z": device(z - 1, y, x, core),
            "X": device(z, y, nx, core),
            "Y": device(z, ny, x, core),
            "P": device(z, y, x, nc),
        }[link]
        ref = gath.at[block, pl.ds(*rows)]
        if link == "P":
            kind = "P0" if kind in PARTNER[:3] else "P1"
        sem = {"Z": planes + d, "P": 2 * planes + 4 + d}.get(link, d)
        if d == 0 and kind in ("XA", "YA", "ZA") and not arriving:
            sem = 2 * planes + (1 if down else 0)
        return pltpu.make_async_remote_copy(
            ref,
            ref,
            send.at[sem],
            recv.at[recvs[kind, d + 1 if down and not arriving else d]],
            device_id=target,
            device_id_type=MESH,
        )

    def multiply(kind, d):
        base, count = (0, 6) if kind == "M0" else (6, 2)

        for i in range(base, base + count):
            block = slot(z + d, ny if i & 4 else y, nx if i & 2 else x, i & 1)
            at = pl.ds(pl.multiple_of(block * width, width), width)
            product = jnp.dot(zt[...], gath[block], preferred_element_type=jnp.float32).astype(jnp.bfloat16)
            if d == 0:
                product = jnp.where(block >= own, product, jnp.bfloat16(0.0))
            out_ref[:, at] = product

    def whole(count, sem, rows=None):
        rows = rows or next(n for n in range(bars, 0, -8) if count % n == 0)
        ref = gath.at[pl.ds(0, count // rows), pl.ds(0, rows)]
        return pltpu.make_async_remote_copy(ref, ref, sem, sem, device_id=device(z, y, x, nc), device_id_type=MESH)

    def act(action, kind, d):
        if action == "multiply":
            multiply(kind, d)
        elif action == "wait" and kind[0] == "P":
            whole((3 if kind == "P0" else 1) * bars, recv.at[recvs[kind, d]]).wait_recv()
        elif action == "wait" and (kind, d) in STATS:
            k = ("XA", "YA", "ZA").index(kind)
            raw_here = z == 0 if k == 2 else z < low
            block = slot(z + d, ny if k == 1 else y, nx if k == 0 else x, core)
            pl.when(raw_here)(lambda: convert(k, block))
            pl.when(jnp.logical_not(raw_here))(lambda: copy(kind, d, True).wait_recv())
        elif action == "wait":
            copy(kind, d, True).wait_recv()
        elif d == 0 and kind in ("XA", "YA", "ZA"):
            k = ("XA", "YA", "ZA").index(kind)
            pl.when(z < low)(lambda: early(k, stats, stat_rows).start())
            pl.when(z >= low)(lambda: copy(kind, d, False).start())
        else:
            copy(kind, d, False).start()

    def guarded(key, run):
        name, d = key
        if name == "sends down":
            pl.when(jnp.minimum(z, planes - z - d) > 0)(run)
        elif d:
            pl.when(z + d < planes)(run)
        else:
            run()

    actions = plan(planes)
    sent = {}
    for action, kind, d in actions:
        if action == "start":
            key = group(action, kind, d)
            if not (d == 0 and kind in ("XA", "YA", "ZA")):
                link, _, rows = piece(kind, d, False)
                key += ({"Z": planes + d, "P": 2 * planes + 4 + d}.get(link, d),)
                sent[key] = sent.get(key, 0) + rows[1]
    transposed = False
    while actions:
        key = group(*actions[0])
        count = 1
        while count < len(actions) and group(*actions[count]) == key:
            count += 1
        batch, actions = actions[:count], actions[count:]

        def run(batch=batch):
            for action in batch:
                act(*action)

        if not transposed and batch[0][0] != "start":
            zt[...] = gath[own].T
            transposed = True
        guarded(key, run)
    for (*key, sem), rows in sent.items():
        guarded(key, lambda rows=rows, sem=sem: whole(rows, send.at[sem]).wait_send())

    @pl.when(z < low)
    def _():
        part_wait(8 * low - 1).wait_send()
        whole(4 * (half + 8), send.at[2 * planes + 2]).wait_send()

    @pl.when(z >= low)
    def _():
        part_wait(8 * low).wait_send()
        whole(2 * half, send.at[2 * planes]).wait_send()
        whole(half, send.at[2 * planes + 1]).wait_send()

    if planes > 1:

        @pl.when(z == 1)
        def _():
            whole(2 * (half + 8), send.at[2 * planes + 3]).wait_send()

    if planes > low:

        @pl.when(z == low - 1)
        def _():
            for zz in range(low, planes):
                total_copy(zz).wait_send()


def shards(planes, returns):
    bars, width = returns.shape
    blocks = planes * 8
    held = blocks * width * (2 * bars + 2 * width) + 6 * bars * width
    products = pl.pallas_call(
        functools.partial(kernel, planes),
        out_shape=jax.ShapeDtypeStruct((width, blocks * width), jnp.bfloat16),
        in_specs=[pl.BlockSpec(memory_space=pltpu.HBM)],
        out_specs=pl.BlockSpec(memory_space=pltpu.VMEM),
        scratch_shapes=[
            pltpu.VMEM((bars, width), jnp.float32),
            pltpu.VMEM((blocks, bars, width), jnp.bfloat16),
            pltpu.VMEM((width, bars), jnp.bfloat16),
            pltpu.VMEM((blocks, 1, bars), jnp.float32),
            pltpu.VMEM((1, bars), jnp.float32),
            pltpu.VMEM((bars, 128), jnp.float32),
            pltpu.VMEM((3, bars * 13 // 32 // 16 * 16 + 8, width), jnp.float32),
            pltpu.VMEM((8, width), jnp.float32),
            pltpu.SemaphoreType.DMA,
            pltpu.SemaphoreType.DMA((2,)),
            pltpu.SemaphoreType.DMA((2,)),
            pltpu.SemaphoreType.DMA((3 * planes + 4,)),
            pltpu.SemaphoreType.DMA((14 * planes - 4,)),
        ],
        compiler_params=pltpu.CompilerParams(
            collective_id=0, has_side_effects=True, vmem_limit_bytes=held + 4 * 1024 * 1024
        ),
    )(pltpu.with_memory_space_constraint(returns, pltpu.HBM))
    return products


def solution(mesh):
    planes = mesh.shape["blk"] // 4
    in_specs = (P(None, ("blk", "grp")),)
    out_specs = P(("blk", "grp"), None)
    return jax.shard_map(
        functools.partial(shards, planes), mesh=mesh, in_specs=in_specs, out_specs=out_specs, check_vma=False
    )
```

```python
import functools
import math

import jax
import jax.numpy as jnp
from jax import lax
from jax.experimental import pallas as pl
from jax.experimental.pallas import tpu as pltpu
from jax.sharding import PartitionSpec as P

MESH = pl.DeviceIdType.MESH
DOWN = ("ZA", "ZB", "ZO", "ZX", "ZY", "ZD")
SPREAD = ("XA", "XB", "YA", "YB", "D0", "D1")
REST = ("XR", "YR")
PARTNER = ("P0", "P1", "P2", "P3", "P4")
KINDS = DOWN + SPREAD + REST
STATS = ("XA", "YA", "ZA")
WAITS_LOW = (
    {
        "XA": 0, "YA": 1, "YB": 3, "YR": 4, "XB": 6, "XR": 7, "D0": 9, "D1": 11,
        "M0": 24, "M1": 27,
    },
    {
        "ZA": 2, "ZO": 5, "ZB": 8, "XA": 12, "YB": 13, "XB": 15, "D0": 18, "YA": 20,
        "ZY": 21, "ZX": 22, "M0": 37, "D1": 40, "ZD": 42, "M1": 46,
    },
    {
        "ZA": 10, "ZB": 14, "YA": 17, "ZO": 23, "XA": 25, "YB": 26, "ZY": 29, "XB": 31,
        "ZX": 38, "D0": 39, "D1": 41, "ZD": 44, "M1": 49, "M0": 50,
    },
    {
        "ZA": 16, "ZB": 19, "ZO": 28, "ZY": 30, "XA": 32, "YA": 33, "YB": 34, "XB": 35,
        "ZX": 36, "M0": 43, "D0": 45, "D1": 47, "ZD": 48, "M1": 51,
    },
)
WAITS_HIGH = (
    {
        "XR": 2, "YB": 3, "YR": 5, "XA": 9, "D1": 17, "D0": 19, "YA": 21, "XB": 26,
        "M0": 27, "M1": 28,
    },
    {
        "ZA": 0, "ZB": 1, "ZO": 7, "ZY": 10, "XA": 12, "XB": 13, "ZX": 16, "ZD": 18,
        "YB": 20, "D0": 25, "YA": 33, "D1": 34, "M0": 36, "M1": 37,
    },
    {
        "ZA": 4, "ZB": 6, "ZO": 8, "ZY": 11, "YA": 14, "ZX": 15, "ZD": 22, "YB": 23,
        "XB": 24, "XA": 29, "D1": 30, "D0": 31, "M0": 32, "M1": 35,
    },
)
PERIOD = 16
SENDS_LOW = (
    "D0", "YR", "D1", "ZD", "YA", "ZX", "ZY", "P4", "P0", "XA",
    "P3", "ZO", "XR", "ZA", "ZB", "YB", "P1", "XB", "P2",
)
SENDS_HIGH = (
    "ZX", "D0", "ZY", "XR", "ZA", "P1", "ZB", "XB", "ZO", "YR",
    "P3", "ZD", "D1", "YB", "P2", "P0", "P4", "XA", "YA",
)

def needs(kind, d):
    first = d == 0
    return {
        "ZA": [] if first else ["ZA"],
        "ZB": [] if first else ["ZB"],
        "ZO": [] if first else ["ZO"],
        "ZX": ["XR"] if first else ["ZX"],
        "ZY": ["YR"] if first else ["ZY"],
        "ZD": ["D1"] if first else ["ZD"],
        "XA": [] if first else ["ZA"],
        "YA": [] if first else ["ZA"],
        "XB": [] if first else ["ZB"],
        "YB": [] if first else ["ZB"],
        "XR": [],
        "YR": [],
        "D0": ["XA"],
        "D1": ["YB", "YR"] if first else ["YB"],
        "P0": [] if first else ["ZA", "ZB", "ZO"],
        "P1": ["XA", "XB", "XR" if first else "ZX"],
        "P2": ["YA", "YB", "YR" if first else "ZY"],
        "P3": ["D0"],
        "P4": ["D1"] if first else ["D1", "ZD"],
    }[kind]


def early_depth(bars):
    return bars * 16 // 32 // 16 * 16


def early_depth(bars):
    return bars * 16 // 32 // 16 * 16


def group(action, kind, d):
    if action == "start" and kind in DOWN:
        return ("sends down", d)
    return ("holds", d)


def plan(planes, lowest):
    waits, sends = (WAITS_LOW, SENDS_LOW) if lowest else (WAITS_HIGH, SENDS_HIGH)
    span = planes if lowest else planes - 1
    events = []
    for d in range(span):
        kinds = SPREAD + (DOWN if d else REST) + ("M0", "M1")
        known = min(d, len(waits) - 1)
        events += [(waits[known][kind] + PERIOD * (d - known), kind, d) for kind in kinds]
    here, sent, actions = set(), set(), []

    def send():
        for d in range(span):
            for kind in sends:
                absent = (kind in REST and d > 0) or (kind in DOWN and lowest)
                if (kind, d) not in sent and not absent and all((k, d) in here for k in needs(kind, d)):
                    sent.add((kind, d))
                    actions.append(("start", kind, d))

    for kind in STATS[:2] if lowest else STATS:
        sent.add((kind, 0))
        actions.append(("start", kind, 0))
    send()
    for _, kind, d in sorted(events):
        if kind in ("M0", "M1"):
            actions.append(("wait", "P" + kind[1], d))
            actions.append(("multiply", kind, d))
        else:
            actions.append(("wait", kind, d))
            here.add((kind, d))
            send()
    return actions


def kernel(
    planes, r_hbm, out_ref, r_ref, gath, zt, parts, total, market, raw, stats, load_sem, psend, precv, send, recv
):
    bars, width = r_ref.shape
    blocks = gath.shape[0]
    low = min(2, planes)
    blk, core = lax.axis_index("blk"), lax.axis_index("grp")
    x, y, z = lax.rem(blk, 2), lax.rem(lax.div(blk, 2), 2), lax.div(blk, 4)
    nx, ny, nc = 1 - x, 1 - y, 1 - core
    high = bars * 25 // 32 // 16 * 16
    half = bars * 13 // 32 // 16 * 16
    early_rows = early_depth(bars)
    rows_r = (high, bars - high)

    def device(zz, yy, xx, cc):
        return {"blk": (zz * 2 + yy) * 2 + xx, "grp": cc}

    def slot(zz, yy, xx, cc):
        return ((zz * 2 + yy) * 2 + xx) * 2 + cc

    own = slot(z, y, x, core)
    load = pltpu.make_async_copy(r_hbm, r_ref, load_sem)
    load.start()
    barrier = pltpu.get_barrier_semaphore()

    def greet(target):
        pl.semaphore_signal(barrier, inc=1, device_id=target, device_id_type=MESH)

    @pl.when(z < low)
    def _():
        for j in range(blocks):
            pl.when(own != j)(functools.partial(greet, {"blk": j // 2, "grp": j % 2}))

    if planes > low + 1:

        @pl.when(jnp.logical_and(z >= low, z < planes - 1))
        def _():
            greet(device(z + 1, y, x, core))

    load.wait()
    lanes = r_ref[:, :128]
    for i in range(1, width // 128):
        lanes = lanes + r_ref[:, 128 * i : 128 * (i + 1)]
    parts[own] = jnp.sum(lanes.T, axis=0, keepdims=True)

    def part_copy(target):
        return pltpu.make_async_remote_copy(
            parts.at[own], parts.at[own], psend, precv, device_id=target, device_id_type=MESH
        )

    def part_wait(count):
        rest = parts.at[pl.ds(0, count)]
        return pltpu.make_async_remote_copy(
            rest, rest, psend, precv, device_id=device(z, y, x, nc), device_id_type=MESH
        )

    def total_copy(zz):
        return pltpu.make_async_remote_copy(
            total, total, psend, precv, device_id=device(zz, y, x, core), device_id_type=MESH
        )

    pl.semaphore_wait(barrier, 8 * low + jnp.where(z < low, -1, 0) + jnp.where(z > low, 1, 0))
    for j in range(8 * low):
        pl.when(own != j)(lambda j=j: part_copy({"blk": j // 2, "grp": j % 2}).start())

    recvs = {}
    for d in range(planes):
        for kind in SPREAD + (DOWN if d else REST) + ("P0", "P1"):
            recvs[kind, d] = len(recvs)

    def early(k, source, rows):
        kind, d, target = (
            ("XA", 0, device(z, y, nx, core)),
            ("YA", 0, device(z, ny, x, core)),
            ("ZA", 1, device(z - 1, y, x, core)),
        )[k]
        return pltpu.make_async_remote_copy(
            source,
            raw.at[k, pl.ds(*rows)],
            send.at[1],
            recv.at[recvs[kind, d]],
            device_id=target,
            device_id_type=MESH,
        )

    depths = (early_rows, early_rows, half)
    deepest = raw.shape[1] - 8

    def early_raw(k):
        early(k, r_ref.at[pl.ds(0, depths[k])], (0, depths[k])).start()

    @pl.when(z < low)
    def _():
        early_raw(0)
        early_raw(1)

    if planes > 1:
        pl.when(z > 0)(lambda: early_raw(2))

    @pl.loop(0, z * 8)
    def _(block):
        at = pl.ds(pl.multiple_of(block * width, width), width)
        out_ref[:, at] = jnp.zeros((width, width), jnp.bfloat16)

    @pl.when(z < low)
    def _():
        part_wait(blocks - 1).wait_recv()
        total[...] = jnp.sum(parts[...], axis=0) * (1.0 / (width * blocks))

    if planes > low:

        @pl.when(z == low - 1)
        def _():
            for zz in range(low, planes):
                total_copy(zz).start()

        pl.when(z >= low)(lambda: total_copy(z).wait_recv())

    market[...] = jnp.broadcast_to(total[...], (128, bars)).T
    first = lax.broadcasted_iota(jnp.int32, (8, 128), 0) == 0
    for i in range(width // 128):
        at = slice(128 * i, 128 * (i + 1))
        excess = r_ref[:, at] - market[...]
        mean = jnp.mean(excess, axis=0, keepdims=True)
        deviation = excess - mean
        inverse = lax.rsqrt(jnp.mean(deviation * deviation, axis=0, keepdims=True) + 1e-06) / math.sqrt(bars)
        stats[:, at] = jnp.where(first, mean, inverse)
        gath[own, :, at] = (deviation * inverse).astype(jnp.bfloat16)

    def convert(k, block):
        depth = depths[k]
        landed = (0, depth + 8)
        early(k, raw.at[k, pl.ds(*landed)], landed).wait_recv()
        for i in range(width // 128):
            at = slice(128 * i, 128 * (i + 1))
            deviation = raw[k, :depth, at] - market[:depth] - raw[k, deepest : deepest + 1, at]
            gath[block, :depth, at] = (deviation * raw[k, deepest + 1 : deepest + 2, at]).astype(jnp.bfloat16)

    def piece(kind, d, arriving):
        link = kind[0] if kind[0] != "D" else ("Y" if kind == "D0" else "X")
        first = early_rows if d == 0 and link != "Z" else half
        rows_a, rows_b = (0, first), (first, high - first)
        if arriving:
            flip = {"X": (0, 1), "Y": (1, 0), "D": (1, 1)}.get(kind[0], (0, 0))
        else:
            flip = {"D0": (0, 1), "D1": (1, 0)}.get(kind, (0, 0))
        if link == "Z":
            flip = {"ZX": (0, 1), "ZY": (1, 0), "ZD": (1, 1)}.get(kind, (0, 0))
            rows = {"ZA": rows_a, "ZB": rows_b}.get(kind, rows_r)
        elif link == "P":
            flip = {"P0": (0, 0), "P1": (0, 1), "P2": (1, 0)}.get(kind, (1, 1))
            rows = {"P3": rows_a, "P4": (first, bars - first)}.get(kind, (0, bars))
        else:
            last = (first, bars - first) if d == 0 else rows_b
            rows = {"A": rows_a, "B": rows_b, "R": rows_r, "0": rows_a, "1": last}[kind[1]]
        return link, flip, rows

    def copy(kind, d, arriving):
        link, flip, rows = piece(kind, d, arriving)
        down = link == "Z"
        block = slot(z + d, ny if flip[0] else y, nx if flip[1] else x, core)
        target = {
            "Z": device(z - 1, y, x, core),
            "X": device(z, y, nx, core),
            "Y": device(z, ny, x, core),
            "P": device(z, y, x, nc),
        }[link]
        ref = gath.at[block, pl.ds(*rows)]
        if link == "P":
            kind = "P0" if kind in PARTNER[:3] else "P1"
        return pltpu.make_async_remote_copy(
            ref,
            ref,
            send.at[0],
            recv.at[recvs[kind, d + 1 if down and not arriving else d]],
            device_id=target,
            device_id_type=MESH,
        )

    def multiply(kind, d):
        base, count = (0, 6) if kind == "M0" else (6, 2)

        for i in range(base, base + count):
            block = slot(z + d, ny if i & 4 else y, nx if i & 2 else x, i & 1)
            at = pl.ds(pl.multiple_of(block * width, width), width)
            product = jnp.dot(zt[...], gath[block], preferred_element_type=jnp.float32).astype(jnp.bfloat16)
            if d == 0:
                product = jnp.where(block >= own, product, jnp.bfloat16(0.0))
            out_ref[:, at] = product

    def whole(count, sem):
        sizes = [n for n in range(8, bars + 1, 8)]
        fits = lambda rows_in_all: [n for n in sizes if rows_in_all % n == 0 and rows_in_all // n <= blocks]
        extra = next(n for n in [0, *sizes] if fits(count - n))
        parts_of = [(count - extra, fits(count - extra)[-1])] + ([(extra, extra)] if extra else [])
        refs = [gath.at[pl.ds(0, number // rows), pl.ds(0, rows)] for number, rows in parts_of]
        partner = device(z, y, x, nc)
        return [
            pltpu.make_async_remote_copy(ref, ref, sem, sem, device_id=partner, device_id_type=MESH) for ref in refs
        ]

    def receive_all(count, sem):
        for part in whole(count, sem):
            part.wait_recv()

    def drain(count, sem):
        for part in whole(count, sem):
            part.wait_send()

    def act(action, kind, d, lowest):
        k = STATS.index(kind) if kind in STATS else 0
        if action == "multiply":
            multiply(kind, d)
        elif action == "wait" and kind[0] == "P":
            receive_all((3 if kind == "P0" else 1) * bars, recv.at[recvs[kind, d]])
        elif action == "wait" and (kind, d) in (("XA", 0), ("YA", 0), ("ZA", 1)):
            block = slot(z + d, ny if k == 1 else y, nx if k == 0 else x, core)
            if lowest or kind == "ZA":
                convert(k, block)
            else:
                pl.when(z < low)(lambda: convert(k, block))
                pl.when(z >= low)(lambda: copy(kind, d, True).wait_recv())
        elif action == "wait":
            copy(kind, d, True).wait_recv()
        elif d == 0 and kind in STATS:
            if lowest or kind == "ZA":
                early(k, stats, (deepest, 8)).start()
            else:
                pl.when(z < low)(lambda: early(k, stats, (deepest, 8)).start())
                pl.when(z >= low)(lambda: copy(kind, d, False).start())
        else:
            copy(kind, d, False).start()

    def carry_out(actions, lowest):
        transposed = False
        while actions:
            name, d = key = group(*actions[0])
            count = 1
            while count < len(actions) and group(*actions[count]) == key:
                count += 1
            batch, actions = actions[:count], actions[count:]

            def run(batch=batch):
                for action in batch:
                    act(*action, lowest)

            if not transposed and batch[0][0] != "start":
                zt[...] = gath[own].T
                transposed = True
            if lowest or d == 0:
                run()
            else:
                pl.when(z + d < planes)(run)

    pl.when(z == 0)(lambda: carry_out(plan(planes, True), True))
    if planes > 1:
        pl.when(z > 0)(lambda: carry_out(plan(planes, False), False))

    def finish(plane):
        count = 0
        for action, kind, d in plan(planes, plane == 0):
            raw_sent = d == 0 and (kind == "ZA" or kind in STATS and plane < low)
            if action == "start" and plane + d < planes and not raw_sent:
                count += piece(kind, d, False)[2][1]
        drain(count, send.at[0])
        raw_rows = (4 * (early_rows + 8) if plane < low else 0) + (2 * (half + 8) if plane else 0)
        drain(raw_rows, send.at[1])
        part_wait(8 * low - (plane < low) + (planes - low if plane == low - 1 else 0)).wait_send()

    for plane in range(planes):
        pl.when(z == plane)(functools.partial(finish, plane))


def shards(planes, returns):
    bars, width = returns.shape
    blocks = planes * 8
    held = blocks * width * (2 * bars + 2 * width) + 6 * bars * width
    products = pl.pallas_call(
        functools.partial(kernel, planes),
        out_shape=jax.ShapeDtypeStruct((width, blocks * width), jnp.bfloat16),
        in_specs=[pl.BlockSpec(memory_space=pltpu.HBM)],
        out_specs=pl.BlockSpec(memory_space=pltpu.VMEM),
        scratch_shapes=[
            pltpu.VMEM((bars, width), jnp.float32),
            pltpu.VMEM((blocks, bars, width), jnp.bfloat16),
            pltpu.VMEM((width, bars), jnp.bfloat16),
            pltpu.VMEM((blocks, 1, bars), jnp.float32),
            pltpu.VMEM((1, bars), jnp.float32),
            pltpu.VMEM((bars, 128), jnp.float32),
            pltpu.VMEM((3, early_depth(bars) + 8, width), jnp.float32),
            pltpu.VMEM((8, width), jnp.float32),
            pltpu.SemaphoreType.DMA,
            pltpu.SemaphoreType.DMA,
            pltpu.SemaphoreType.DMA,
            pltpu.SemaphoreType.DMA((2,)),
            pltpu.SemaphoreType.DMA((14 * planes - 4,)),
        ],
        compiler_params=pltpu.CompilerParams(
            collective_id=0, has_side_effects=True, vmem_limit_bytes=held + 4 * 1024 * 1024
        ),
    )(pltpu.with_memory_space_constraint(returns, pltpu.HBM))
    return products


def solution(mesh):
    planes = mesh.shape["blk"] // 4
    in_specs = (P(None, ("blk", "grp")),)
    out_specs = P(("blk", "grp"), None)
    return jax.shard_map(
        functools.partial(shards, planes), mesh=mesh, in_specs=in_specs, out_specs=out_specs, check_vma=False
    )
```

```python
import functools
import math

import jax
import jax.numpy as jnp
from jax import lax
from jax.experimental import pallas as pl
from jax.experimental.pallas import tpu as pltpu
from jax.sharding import PartitionSpec as P

MESH = pl.DeviceIdType.MESH
DOWN = ("ZA", "ZB", "ZO", "ZX", "ZY", "ZD")
SPREAD = ("XA", "XB", "YA", "YB", "D0", "D1")
REST = ("XR", "YR")
PARTNER = ("P0", "P1", "P2", "P3", "P4")
KINDS = DOWN + SPREAD + REST
STATS = ("XA", "YA", "ZA")
WAITS_LOW = (
    {
        "XA": 0, "YA": 1, "YB": 3, "YR": 4, "XB": 6, "XR": 7, "D0": 9, "D1": 11,
        "M0": 24, "M1": 27,
    },
    {
        "ZA": 2, "ZO": 5, "ZB": 8, "XA": 12, "YB": 13, "XB": 15, "D0": 18, "YA": 20,
        "ZY": 21, "ZX": 22, "M0": 37, "D1": 40, "ZD": 42, "M1": 49,
    },
    {
        "ZA": 10, "ZB": 14, "YA": 17, "ZO": 23, "XA": 25, "YB": 26, "ZY": 29, "XB": 31,
        "ZX": 38, "D0": 39, "D1": 41, "ZD": 44, "M0": 45, "M1": 50,
    },
    {
        "ZA": 16, "ZB": 19, "ZO": 28, "ZY": 30, "XA": 32, "YA": 33, "YB": 34, "XB": 35,
        "ZX": 36, "M0": 43, "D0": 46, "D1": 47, "ZD": 48, "M1": 51,
    },
)
WAITS_HIGH = (
    {
        "XR": 2, "YB": 3, "YR": 5, "XA": 9, "D1": 17, "D0": 19, "YA": 21, "XB": 26,
        "M0": 27, "M1": 28,
    },
    {
        "ZA": 0, "ZB": 1, "ZO": 7, "ZY": 10, "XA": 12, "XB": 13, "ZX": 16, "ZD": 18,
        "YB": 20, "D0": 25, "YA": 33, "D1": 34, "M0": 36, "M1": 37,
    },
    {
        "ZA": 4, "ZB": 6, "ZO": 8, "ZY": 11, "YA": 14, "ZX": 15, "ZD": 22, "YB": 23,
        "XB": 24, "XA": 29, "D1": 30, "D0": 31, "M0": 32, "M1": 35,
    },
)
PERIOD = 16
SENDS_LOW = (
    "D0", "YR", "D1", "ZD", "YA", "ZX", "ZY", "P4", "P0", "XA",
    "P3", "ZO", "XR", "ZA", "ZB", "YB", "P1", "XB", "P2",
)
SENDS_HIGH = (
    "ZX", "D0", "ZY", "XR", "ZA", "P1", "ZB", "XB", "ZO", "YR",
    "P3", "ZD", "D1", "YB", "P2", "P0", "P4", "XA", "YA",
)

def needs(kind, d):
    first = d == 0
    return {
        "ZA": [] if first else ["ZA"],
        "ZB": [] if first else ["ZB"],
        "ZO": [] if first else ["ZO"],
        "ZX": ["XR"] if first else ["ZX"],
        "ZY": ["YR"] if first else ["ZY"],
        "ZD": ["D1"] if first else ["ZD"],
        "XA": [] if first else ["ZA"],
        "YA": [] if first else ["ZA"],
        "XB": [] if first else ["ZB"],
        "YB": [] if first else ["ZB"],
        "XR": [],
        "YR": [],
        "D0": ["XA"],
        "D1": ["YB", "YR"] if first else ["YB"],
        "P0": [] if first else ["ZA", "ZB", "ZO"],
        "P1": ["XA", "XB", "XR" if first else "ZX"],
        "P2": ["YA", "YB", "YR" if first else "ZY"],
        "P3": ["D0"],
        "P4": ["D1"] if first else ["D1", "ZD"],
    }[kind]


def early_depth(bars):
    return bars * 16 // 32 // 16 * 16


def early_depth(bars):
    return bars * 16 // 32 // 16 * 16


def group(action, kind, d):
    if action == "start" and kind in DOWN:
        return ("sends down", d)
    return ("holds", d)


def plan(planes, lowest):
    waits, sends = (WAITS_LOW, SENDS_LOW) if lowest else (WAITS_HIGH, SENDS_HIGH)
    span = planes if lowest else planes - 1
    events = []
    for d in range(span):
        kinds = SPREAD + (DOWN if d else REST) + ("M0", "M1")
        known = min(d, len(waits) - 1)
        events += [(waits[known][kind] + PERIOD * (d - known), kind, d) for kind in kinds]
    here, sent, actions = set(), set(), []

    def send():
        for d in range(span):
            for kind in sends:
                absent = (kind in REST and d > 0) or (kind in DOWN and lowest)
                if (kind, d) not in sent and not absent and all((k, d) in here for k in needs(kind, d)):
                    sent.add((kind, d))
                    actions.append(("start", kind, d))

    for kind in STATS[:2] if lowest else STATS:
        sent.add((kind, 0))
        actions.append(("start", kind, 0))
    send()
    for _, kind, d in sorted(events):
        if kind in ("M0", "M1"):
            actions.append(("wait", "P" + kind[1], d))
            actions.append(("multiply", kind, d))
        else:
            actions.append(("wait", kind, d))
            here.add((kind, d))
            send()
    return actions


def kernel(
    planes, r_hbm, out_ref, gath, zt, r_ref, parts, total, market, raw, stats, load_sem, psend, precv, send, recv
):
    bars, width = r_ref.shape
    blocks = gath.shape[0]
    low = min(2, planes)
    blk, core = lax.axis_index("blk"), lax.axis_index("grp")
    x, y, z = lax.rem(blk, 2), lax.rem(lax.div(blk, 2), 2), lax.div(blk, 4)
    nx, ny, nc = 1 - x, 1 - y, 1 - core
    high = bars * 25 // 32 // 16 * 16
    half = bars * 13 // 32 // 16 * 16
    early_rows = early_depth(bars)
    rows_r = (high, bars - high)

    def device(zz, yy, xx, cc):
        return {"blk": (zz * 2 + yy) * 2 + xx, "grp": cc}

    def slot(zz, yy, xx, cc):
        return ((zz * 2 + yy) * 2 + xx) * 2 + cc

    own = slot(z, y, x, core)
    load = pltpu.make_async_copy(r_hbm, r_ref, load_sem)
    load.start()
    barrier = pltpu.get_barrier_semaphore()

    def greet(target):
        pl.semaphore_signal(barrier, inc=1, device_id=target, device_id_type=MESH)

    @pl.when(z < low)
    def _():
        for j in range(blocks):
            pl.when(own != j)(functools.partial(greet, {"blk": j // 2, "grp": j % 2}))

    if planes > low + 1:

        @pl.when(jnp.logical_and(z >= low, z < planes - 1))
        def _():
            greet(device(z + 1, y, x, core))

    load.wait()
    lanes = r_ref[:, :128]
    for i in range(1, width // 128):
        lanes = lanes + r_ref[:, 128 * i : 128 * (i + 1)]
    parts[own] = jnp.sum(lanes.T, axis=0, keepdims=True)

    def part_copy(target):
        return pltpu.make_async_remote_copy(
            parts.at[own], parts.at[own], psend, precv, device_id=target, device_id_type=MESH
        )

    def part_wait(count):
        rest = parts.at[pl.ds(0, count)]
        return pltpu.make_async_remote_copy(
            rest, rest, psend, precv, device_id=device(z, y, x, nc), device_id_type=MESH
        )

    def total_copy(zz):
        return pltpu.make_async_remote_copy(
            total, total, psend, precv, device_id=device(zz, y, x, core), device_id_type=MESH
        )

    pl.semaphore_wait(barrier, 8 * low + jnp.where(z < low, -1, 0) + jnp.where(z > low, 1, 0))
    for j in range(8 * low):
        pl.when(own != j)(lambda j=j: part_copy({"blk": j // 2, "grp": j % 2}).start())

    recvs = {}
    for d in range(planes):
        for kind in SPREAD + (DOWN if d else REST) + ("P0", "P1"):
            recvs[kind, d] = len(recvs)

    def early(k, source, rows):
        kind, d, target = (
            ("XA", 0, device(z, y, nx, core)),
            ("YA", 0, device(z, ny, x, core)),
            ("ZA", 1, device(z - 1, y, x, core)),
        )[k]
        return pltpu.make_async_remote_copy(
            source,
            raw.at[k, pl.ds(*rows)],
            send.at[1],
            recv.at[recvs[kind, d]],
            device_id=target,
            device_id_type=MESH,
        )

    depths = (early_rows, early_rows, half)
    deepest = raw.shape[1] - 8

    def early_raw(k):
        early(k, r_ref.at[pl.ds(0, depths[k])], (0, depths[k])).start()

    @pl.when(z < low)
    def _():
        early_raw(0)
        early_raw(1)

    if planes > 1:
        pl.when(z > 0)(lambda: early_raw(2))

    @pl.loop(0, z * 8)
    def _(block):
        at = pl.ds(pl.multiple_of(block * width, width), width)
        out_ref[:, at] = jnp.zeros((width, width), jnp.bfloat16)

    @pl.when(z < low)
    def _():
        part_wait(blocks - 1).wait_recv()
        total[...] = jnp.sum(parts[...], axis=0) * (1.0 / (width * blocks))

    if planes > low:

        @pl.when(z == low - 1)
        def _():
            for zz in range(low, planes):
                total_copy(zz).start()

        pl.when(z >= low)(lambda: total_copy(z).wait_recv())

    market[...] = jnp.broadcast_to(total[...], (128, bars)).T
    first = lax.broadcasted_iota(jnp.int32, (8, 128), 0) == 0
    for i in range(width // 128):
        at = slice(128 * i, 128 * (i + 1))
        excess = r_ref[:, at] - market[...]
        mean = jnp.mean(excess, axis=0, keepdims=True)
        deviation = excess - mean
        inverse = lax.rsqrt(jnp.mean(deviation * deviation, axis=0, keepdims=True) + 1e-06) / math.sqrt(bars)
        stats[:, at] = jnp.where(first, mean, inverse)
        gath[own, :, at] = (deviation * inverse).astype(jnp.bfloat16)

    def convert(k, block):
        depth = depths[k]
        landed = (0, depth + 8)
        early(k, raw.at[k, pl.ds(*landed)], landed).wait_recv()
        for i in range(width // 128):
            at = slice(128 * i, 128 * (i + 1))
            deviation = raw[k, :depth, at] - market[:depth] - raw[k, deepest : deepest + 1, at]
            gath[block, :depth, at] = (deviation * raw[k, deepest + 1 : deepest + 2, at]).astype(jnp.bfloat16)

    def piece(kind, d, arriving):
        link = kind[0] if kind[0] != "D" else ("Y" if kind == "D0" else "X")
        first = early_rows if d == 0 and link != "Z" else half
        rows_a, rows_b = (0, first), (first, high - first)
        if arriving:
            flip = {"X": (0, 1), "Y": (1, 0), "D": (1, 1)}.get(kind[0], (0, 0))
        else:
            flip = {"D0": (0, 1), "D1": (1, 0)}.get(kind, (0, 0))
        if link == "Z":
            flip = {"ZX": (0, 1), "ZY": (1, 0), "ZD": (1, 1)}.get(kind, (0, 0))
            rows = {"ZA": rows_a, "ZB": rows_b}.get(kind, rows_r)
        elif link == "P":
            flip = {"P0": (0, 0), "P1": (0, 1), "P2": (1, 0)}.get(kind, (1, 1))
            rows = {"P3": rows_a, "P4": (first, bars - first)}.get(kind, (0, bars))
        else:
            last = (first, bars - first) if d == 0 else rows_b
            rows = {"A": rows_a, "B": rows_b, "R": rows_r, "0": rows_a, "1": last}[kind[1]]
        return link, flip, rows

    def copy(kind, d, arriving):
        link, flip, rows = piece(kind, d, arriving)
        down = link == "Z"
        block = slot(z + d, ny if flip[0] else y, nx if flip[1] else x, core)
        target = {
            "Z": device(z - 1, y, x, core),
            "X": device(z, y, nx, core),
            "Y": device(z, ny, x, core),
            "P": device(z, y, x, nc),
        }[link]
        ref = gath.at[block, pl.ds(*rows)]
        if link == "P":
            kind = "P0" if kind in PARTNER[:3] else "P1"
        return pltpu.make_async_remote_copy(
            ref,
            ref,
            send.at[0],
            recv.at[recvs[kind, d + 1 if down and not arriving else d]],
            device_id=target,
            device_id_type=MESH,
        )

    def multiply(kind, d):
        base, count = (0, 6) if kind == "M0" else (6, 2)

        for i in range(base, base + count):
            block = slot(z + d, ny if i & 4 else y, nx if i & 2 else x, i & 1)
            at = pl.ds(pl.multiple_of(block * width, width), width)
            product = jnp.dot(zt[...], gath[block], preferred_element_type=jnp.float32).astype(jnp.bfloat16)
            if d == 0:
                product = jnp.where(block >= own, product, jnp.bfloat16(0.0))
            out_ref[:, at] = product

    def whole(count, sem):
        sizes = [n for n in range(8, bars + 1, 8)]
        fits = lambda rows_in_all: [n for n in sizes if rows_in_all % n == 0 and rows_in_all // n <= blocks]
        extra = next(n for n in [0, *sizes] if fits(count - n))
        parts_of = [(count - extra, fits(count - extra)[-1])] + ([(extra, extra)] if extra else [])
        refs = [gath.at[pl.ds(0, number // rows), pl.ds(0, rows)] for number, rows in parts_of]
        partner = device(z, y, x, nc)
        return [
            pltpu.make_async_remote_copy(ref, ref, sem, sem, device_id=partner, device_id_type=MESH) for ref in refs
        ]

    def receive_all(count, sem):
        for part in whole(count, sem):
            part.wait_recv()

    def drain(count, sem):
        for part in whole(count, sem):
            part.wait_send()

    def act(action, kind, d, lowest):
        k = STATS.index(kind) if kind in STATS else 0
        if action == "multiply" and lowest:
            if d < planes - 1:
                multiply(kind, d)
        elif action == "multiply":
            pl.when(z + d < planes - 1)(lambda: multiply(kind, d))
        elif action == "wait" and kind[0] == "P":
            receive_all((3 if kind == "P0" else 1) * bars, recv.at[recvs[kind, d]])
        elif action == "wait" and (kind, d) in (("XA", 0), ("YA", 0), ("ZA", 1)):
            block = slot(z + d, ny if k == 1 else y, nx if k == 0 else x, core)
            if lowest or kind == "ZA":
                convert(k, block)
            else:
                pl.when(z < low)(lambda: convert(k, block))
                pl.when(z >= low)(lambda: copy(kind, d, True).wait_recv())
        elif action == "wait":
            copy(kind, d, True).wait_recv()
        elif d == 0 and kind in STATS:
            if lowest or kind == "ZA":
                early(k, stats, (deepest, 8)).start()
            else:
                pl.when(z < low)(lambda: early(k, stats, (deepest, 8)).start())
                pl.when(z >= low)(lambda: copy(kind, d, False).start())
        else:
            copy(kind, d, False).start()

    def carry_out(actions, lowest):
        transposed = False
        while actions:
            name, d = key = group(*actions[0])
            count = 1
            while count < len(actions) and group(*actions[count]) == key:
                count += 1
            batch, actions = actions[:count], actions[count:]

            def run(batch=batch):
                for action in batch:
                    act(*action, lowest)

            if not transposed and batch[0][0] != "start":
                zt[...] = gath[own].T
                transposed = True
            if lowest or d == 0:
                run()
            else:
                pl.when(z + d < planes)(run)

    pl.when(z == 0)(lambda: carry_out(plan(planes, True), True))
    if planes > 1:
        pl.when(z > 0)(lambda: carry_out(plan(planes, False), False))

    def finish(plane):
        count = 0
        for action, kind, d in plan(planes, plane == 0):
            raw_sent = d == 0 and (kind == "ZA" or kind in STATS and plane < low)
            if action == "start" and plane + d < planes and not raw_sent:
                count += piece(kind, d, False)[2][1]
        drain(count, send.at[0])
        raw_rows = (4 * (early_rows + 8) if plane < low else 0) + (2 * (half + 8) if plane else 0)
        drain(raw_rows, send.at[1])
        part_wait(8 * low - (plane < low) + (planes - low if plane == low - 1 else 0)).wait_send()

    for plane in range(planes):
        pl.when(z == plane)(functools.partial(finish, plane))


def finish_kernel(early_ref, gath, zt, out_hbm, late_ref, sem):
    blocks, _, width = gath.shape
    own = lax.axis_index("blk") * 2 + lax.axis_index("grp")
    ready = width * (blocks - 8)
    copies = [pltpu.make_async_copy(early_ref, out_hbm.at[:, pl.ds(0, ready)], sem.at[0])]
    copies[0].start()
    for i in range(8):
        block = blocks - 8 + i
        product = jnp.dot(zt[...], gath[block], preferred_element_type=jnp.float32).astype(jnp.bfloat16)
        late_ref[:, width * i : width * (i + 1)] = jnp.where(block >= own, product, jnp.bfloat16(0.0))
        if i % 4 == 3:
            at = pl.ds(width * (i - 3), 4 * width)
            to = pl.ds(ready + width * (i - 3), 4 * width)
            copies.append(pltpu.make_async_copy(late_ref.at[:, at], out_hbm.at[:, to], sem.at[len(copies)]))
            copies[-1].start()
    for copy in copies:
        copy.wait()


def shards(planes, returns):
    bars, width = returns.shape
    blocks = planes * 8
    held = blocks * width * (2 * bars + 2 * width) + 6 * bars * width
    vmem = pl.BlockSpec(memory_space=pltpu.VMEM)
    products, gathered, transposed = pl.pallas_call(
        functools.partial(kernel, planes),
        out_shape=[
            jax.ShapeDtypeStruct((width, (blocks - 8) * width), jnp.bfloat16),
            jax.ShapeDtypeStruct((blocks, bars, width), jnp.bfloat16),
            jax.ShapeDtypeStruct((width, bars), jnp.bfloat16),
        ],
        in_specs=[pl.BlockSpec(memory_space=pltpu.HBM)],
        out_specs=[vmem, vmem, vmem],
        scratch_shapes=[
            pltpu.VMEM((bars, width), jnp.float32),
            pltpu.VMEM((blocks, 1, bars), jnp.float32),
            pltpu.VMEM((1, bars), jnp.float32),
            pltpu.VMEM((bars, 128), jnp.float32),
            pltpu.VMEM((3, early_depth(bars) + 8, width), jnp.float32),
            pltpu.VMEM((8, width), jnp.float32),
            pltpu.SemaphoreType.DMA,
            pltpu.SemaphoreType.DMA,
            pltpu.SemaphoreType.DMA,
            pltpu.SemaphoreType.DMA((2,)),
            pltpu.SemaphoreType.DMA((14 * planes - 4,)),
        ],
        compiler_params=pltpu.CompilerParams(
            collective_id=0, has_side_effects=True, vmem_limit_bytes=held + 4 * 1024 * 1024
        ),
    )(pltpu.with_memory_space_constraint(returns, pltpu.HBM))
    return pl.pallas_call(
        finish_kernel,
        out_shape=jax.ShapeDtypeStruct((width, blocks * width), jnp.bfloat16),
        in_specs=[vmem, vmem, vmem],
        out_specs=pl.BlockSpec(memory_space=pltpu.HBM),
        scratch_shapes=[pltpu.VMEM((width, 8 * width), jnp.bfloat16), pltpu.SemaphoreType.DMA((3,))],
        compiler_params=pltpu.CompilerParams(vmem_limit_bytes=4 * 1024 * 1024),
    )(*(pltpu.with_memory_space_constraint(a, pltpu.VMEM) for a in (products, gathered, transposed)))


def solution(mesh):
    planes = mesh.shape["blk"] // 4
    in_specs = (P(None, ("blk", "grp")),)
    out_specs = P(("blk", "grp"), None)
    return jax.shard_map(
        functools.partial(shards, planes), mesh=mesh, in_specs=in_specs, out_specs=out_specs, check_vma=False
    )
```

```python
import functools
import math

import jax
import jax.numpy as jnp
from jax import lax
from jax.experimental import pallas as pl
from jax.experimental.pallas import tpu as pltpu
from jax.sharding import PartitionSpec as P

MESH = pl.DeviceIdType.MESH
DOWN = ("ZA", "ZB", "ZO", "ZX", "ZY", "ZD")
SPREAD = ("XA", "XB", "YA", "YB", "D0", "D1")
REST = ("XR", "YR")
PARTNER = ("P0", "P1", "P2", "P3", "P4", "P5")
KINDS = DOWN + SPREAD + REST
STATS = ("XA", "YA", "ZA")
HIGHS = (24, 26)
WAITS_LOW = (
    {
        "XA": 0, "YA": 1, "YB": 3, "YR": 4, "XB": 6, "XR": 7, "D0": 9, "D1": 11,
        "M0": 24, "M1": 27,
    },
    {
        "ZA": 2, "ZO": 5, "ZB": 8, "XA": 12, "YB": 13, "XB": 15, "D0": 18, "YA": 20,
        "ZY": 21, "ZX": 22, "M0": 37, "D1": 40, "ZD": 42, "M1": 49,
    },
    {
        "ZA": 10, "ZB": 14, "YA": 17, "ZO": 23, "XA": 25, "YB": 26, "ZY": 29, "XB": 31,
        "ZX": 38, "D0": 39, "D1": 41, "ZD": 44, "M0": 45, "M1": 50,
    },
    {
        "ZA": 16, "ZB": 19, "ZO": 28, "ZY": 30, "XA": 32, "YA": 33, "YB": 34, "XB": 35,
        "ZX": 36, "M0": 43, "D0": 46, "D1": 47, "ZD": 48, "M1": 51,
    },
)
WAITS_HIGH = (
    {
        "XR": 2, "YB": 3, "YR": 5, "XA": 9, "D1": 17, "D0": 19, "YA": 21, "XB": 26,
        "M0": 27, "M1": 28,
    },
    {
        "ZA": 0, "ZB": 1, "ZO": 7, "ZY": 10, "XA": 12, "XB": 13, "ZX": 16, "ZD": 18,
        "YB": 20, "D0": 25, "YA": 33, "D1": 34, "M0": 36, "M1": 37,
    },
    {
        "ZA": 4, "ZB": 6, "ZO": 8, "ZY": 11, "YA": 14, "ZX": 15, "ZD": 22, "YB": 23,
        "XB": 24, "XA": 29, "D1": 30, "D0": 31, "M0": 32, "M1": 35,
    },
)
PERIOD = 16
SENDS_LOW = (
    "P5", "D0", "YR", "D1", "ZD", "YA", "ZX", "ZY", "P4", "P0",
    "XA", "P3", "ZO", "XR", "ZA", "ZB", "YB", "P1", "XB", "P2",
)
SENDS_HIGH = (
    "P5", "ZX", "D0", "ZY", "XR", "ZA", "P1", "ZB", "XB", "ZO",
    "YR", "P3", "ZD", "D1", "YB", "P2", "P0", "P4", "XA", "YA",
)

def needs(kind, d):
    first = d == 0
    return {
        "ZA": [] if first else ["ZA"],
        "ZB": [] if first else ["ZA", "ZB"],
        "ZO": [] if first else ["ZO"],
        "ZX": ["XR"] if first else ["ZX"],
        "ZY": ["YR"] if first else ["ZY"],
        "ZD": ["D1"] if first else ["ZD"],
        "XA": [] if first else ["ZA"],
        "YA": [] if first else ["ZA"],
        "XB": [] if first else ["ZA", "ZB"],
        "YB": [] if first else ["ZA", "ZB"],
        "XR": [],
        "YR": [],
        "D0": ["XA"],
        "D1": ["YB", "YR"] if first else ["YB"],
        "P0": [] if first else ["ZA", "ZB", "ZO"],
        "P1": ["XA", "XB", "XR" if first else "ZX"],
        "P2": ["YA", "YB", "YR" if first else "ZY"],
        "P3": ["D0"],
        "P4": ["D1"],
        "P5": ["ZD"],
    }[kind]


def early_depth(bars):
    return bars * 14 // 32 // 16 * 16


def early_depth(bars):
    return bars * 14 // 32 // 16 * 16


def down_depth(bars):
    return bars * 15 // 32 // 16 * 16


def group(action, kind, d):
    if action == "start" and kind in DOWN:
        return ("sends down", d)
    return ("holds", d)


def plan(planes, lowest):
    waits, sends = (WAITS_LOW, SENDS_LOW) if lowest else (WAITS_HIGH, SENDS_HIGH)
    span = planes if lowest else planes - 1
    events = []
    for d in range(span):
        kinds = SPREAD + (DOWN if d else REST) + ("M0", "M1")
        known = min(d, len(waits) - 1)
        events += [(waits[known][kind] + PERIOD * (d - known), kind, d) for kind in kinds]
    here, sent, actions = set(), set(), []

    def send():
        for d in range(span):
            for kind in sends:
                absent = (kind in REST and d > 0) or (kind in DOWN and lowest) or (kind == "P5" and d == 0)
                if (kind, d) not in sent and not absent and all((k, d) in here for k in needs(kind, d)):
                    sent.add((kind, d))
                    actions.append(("start", kind, d))

    for kind in STATS[:2] if lowest else STATS:
        sent.add((kind, 0))
        actions.append(("start", kind, 0))
    send()
    for _, kind, d in sorted(events):
        if kind in ("M0", "M1"):
            actions.append(("wait", "P" + kind[1], d))
            actions.append(("multiply", kind, d))
        else:
            actions.append(("wait", kind, d))
            here.add((kind, d))
            send()
    return actions


def kernel(
    planes, r_hbm, out_ref, gath, zt, r_ref, parts, total, market, raw, stats, load_sem, psend, precv, send, recv
):
    bars, width = r_ref.shape
    blocks = gath.shape[0]
    low = min(2, planes)
    blk, core = lax.axis_index("blk"), lax.axis_index("grp")
    x, y, z = lax.rem(blk, 2), lax.rem(lax.div(blk, 2), 2), lax.div(blk, 4)
    nx, ny, nc = 1 - x, 1 - y, 1 - core
    highs = tuple(bars * n // 32 // 16 * 16 for n in HIGHS)
    half = bars * 13 // 32 // 16 * 16
    early_rows = early_depth(bars)

    def device(zz, yy, xx, cc):
        return {"blk": (zz * 2 + yy) * 2 + xx, "grp": cc}

    def slot(zz, yy, xx, cc):
        return ((zz * 2 + yy) * 2 + xx) * 2 + cc

    own = slot(z, y, x, core)
    load = pltpu.make_async_copy(r_hbm, r_ref, load_sem)
    load.start()
    barrier = pltpu.get_barrier_semaphore()

    def greet(target):
        pl.semaphore_signal(barrier, inc=1, device_id=target, device_id_type=MESH)

    @pl.when(z < low)
    def _():
        for j in range(blocks):
            pl.when(own != j)(functools.partial(greet, {"blk": j // 2, "grp": j % 2}))

    if planes > low + 1:

        @pl.when(jnp.logical_and(z >= low, z < planes - 1))
        def _():
            greet(device(z + 1, y, x, core))

    load.wait()
    lanes = r_ref[:, :128]
    for i in range(1, width // 128):
        lanes = lanes + r_ref[:, 128 * i : 128 * (i + 1)]
    parts[own] = jnp.sum(lanes.T, axis=0, keepdims=True)

    def part_copy(target):
        return pltpu.make_async_remote_copy(
            parts.at[own], parts.at[own], psend, precv, device_id=target, device_id_type=MESH
        )

    def part_wait(count):
        rest = parts.at[pl.ds(0, count)]
        return pltpu.make_async_remote_copy(
            rest, rest, psend, precv, device_id=device(z, y, x, nc), device_id_type=MESH
        )

    def total_copy(zz):
        return pltpu.make_async_remote_copy(
            total, total, psend, precv, device_id=device(zz, y, x, core), device_id_type=MESH
        )

    pl.semaphore_wait(barrier, 8 * low + jnp.where(z < low, -1, 0) + jnp.where(z > low, 1, 0))
    for j in range(8 * low):
        pl.when(own != j)(lambda j=j: part_copy({"blk": j // 2, "grp": j % 2}).start())

    recvs = {}
    for d in range(planes):
        for kind in SPREAD + (DOWN if d else REST) + ("P0", "P1"):
            recvs[kind, d] = len(recvs)

    def early(k, source, rows):
        kind, d, target = (
            ("XA", 0, device(z, y, nx, core)),
            ("YA", 0, device(z, ny, x, core)),
            ("ZA", 1, device(z - 1, y, x, core)),
        )[k]
        return pltpu.make_async_remote_copy(
            source,
            raw.at[k, pl.ds(*rows)],
            send.at[1],
            recv.at[recvs[kind, d]],
            device_id=target,
            device_id_type=MESH,
        )

    depths = (early_rows, early_rows, down_depth(bars))
    deepest = raw.shape[1] - 8

    def early_raw(k):
        early(k, r_ref.at[pl.ds(0, depths[k])], (0, depths[k])).start()

    @pl.when(z < low)
    def _():
        early_raw(0)
        early_raw(1)

    if planes > 1:
        pl.when(z > 0)(lambda: early_raw(2))

    @pl.loop(0, z * 8)
    def _(block):
        at = pl.ds(pl.multiple_of(block * width, width), width)
        out_ref[:, at] = jnp.zeros((width, width), jnp.bfloat16)

    @pl.when(z < low)
    def _():
        part_wait(blocks - 1).wait_recv()
        total[...] = jnp.sum(parts[...], axis=0) * (1.0 / (width * blocks))

    if planes > low:

        @pl.when(z == low - 1)
        def _():
            for zz in range(low, planes):
                total_copy(zz).start()

        pl.when(z >= low)(lambda: total_copy(z).wait_recv())

    market[...] = jnp.broadcast_to(total[...], (128, bars)).T
    first = lax.broadcasted_iota(jnp.int32, (8, 128), 0) == 0
    for i in range(width // 128):
        at = slice(128 * i, 128 * (i + 1))
        excess = r_ref[:, at] - market[...]
        mean = jnp.mean(excess, axis=0, keepdims=True)
        deviation = excess - mean
        inverse = lax.rsqrt(jnp.mean(deviation * deviation, axis=0, keepdims=True) + 1e-06) / math.sqrt(bars)
        stats[:, at] = jnp.where(first, mean, inverse)
        gath[own, :, at] = (deviation * inverse).astype(jnp.bfloat16)

    def convert(k, block):
        depth = depths[k]
        landed = (0, depth + 8)
        early(k, raw.at[k, pl.ds(*landed)], landed).wait_recv()
        for i in range(width // 128):
            at = slice(128 * i, 128 * (i + 1))
            deviation = raw[k, :depth, at] - market[:depth] - raw[k, deepest : deepest + 1, at]
            gath[block, :depth, at] = (deviation * raw[k, deepest + 1 : deepest + 2, at]).astype(jnp.bfloat16)

    def piece(kind, d, arriving, high):
        link = kind[0] if kind[0] != "D" else ("Y" if kind == "D0" else "X")
        first = half
        if link == "Z" and d == int(arriving):
            first = down_depth(bars)
        elif link != "Z" and d == 0:
            first = early_rows
        rows_a, rows_b, rows_r = (0, first), (first, high - first), (high, bars - high)
        if arriving:
            flip = {"X": (0, 1), "Y": (1, 0), "D": (1, 1)}.get(kind[0], (0, 0))
        else:
            flip = {"D0": (0, 1), "D1": (1, 0)}.get(kind, (0, 0))
        if link == "Z":
            flip = {"ZX": (0, 1), "ZY": (1, 0), "ZD": (1, 1)}.get(kind, (0, 0))
            rows = {"ZA": rows_a, "ZB": rows_b}.get(kind, rows_r)
        elif link == "P":
            flip = {"P0": (0, 0), "P1": (0, 1), "P2": (1, 0)}.get(kind, (1, 1))
            rows = {"P3": rows_a, "P4": rows_b if d else (first, bars - first), "P5": rows_r}.get(kind, (0, bars))
        else:
            last = (first, bars - first) if d == 0 else rows_b
            rows = {"A": rows_a, "B": rows_b, "R": rows_r, "0": rows_a, "1": last}[kind[1]]
        return link, flip, rows

    def copy(kind, d, arriving, run):
        if piece(kind, d, arriving, highs[0]) == piece(kind, d, arriving, highs[1]):
            run(core_copy(kind, d, arriving, highs[0]))
        else:
            for c in range(2):
                pl.when(core == c)(lambda c=c: run(core_copy(kind, d, arriving, highs[c])))

    def core_copy(kind, d, arriving, high):
        link, flip, rows = piece(kind, d, arriving, high)
        down = link == "Z"
        block = slot(z + d, ny if flip[0] else y, nx if flip[1] else x, core)
        target = {
            "Z": device(z - 1, y, x, core),
            "X": device(z, y, nx, core),
            "Y": device(z, ny, x, core),
            "P": device(z, y, x, nc),
        }[link]
        ref = gath.at[block, pl.ds(*rows)]
        if link == "P":
            kind = "P0" if kind in PARTNER[:3] else "P1"
        return pltpu.make_async_remote_copy(
            ref,
            ref,
            send.at[0],
            recv.at[recvs[kind, d + 1 if down and not arriving else d]],
            device_id=target,
            device_id_type=MESH,
        )

    def multiply(kind, d):
        base, count = (0, 6) if kind == "M0" else (6, 2)

        for i in range(base, base + count):
            block = slot(z + d, ny if i & 4 else y, nx if i & 2 else x, i & 1)
            at = pl.ds(pl.multiple_of(block * width, width), width)
            product = jnp.dot(zt[...], gath[block], preferred_element_type=jnp.float32).astype(jnp.bfloat16)
            if d == 0:
                product = jnp.where(block >= own, product, jnp.bfloat16(0.0))
            out_ref[:, at] = product

    def whole(count, sem):
        sizes = [n for n in range(8, bars + 1, 8)]
        fits = lambda rows_in_all: [n for n in sizes if rows_in_all % n == 0 and rows_in_all // n <= blocks]
        extra = next(n for n in [0, *sizes] if fits(count - n))
        parts_of = [(count - extra, fits(count - extra)[-1])] + ([(extra, extra)] if extra else [])
        refs = [gath.at[pl.ds(0, number // rows), pl.ds(0, rows)] for number, rows in parts_of]
        partner = device(z, y, x, nc)
        return [
            pltpu.make_async_remote_copy(ref, ref, sem, sem, device_id=partner, device_id_type=MESH) for ref in refs
        ]

    def receive_all(count, sem):
        for part in whole(count, sem):
            part.wait_recv()

    def drain(count, sem):
        for part in whole(count, sem):
            part.wait_send()

    def act(action, kind, d, lowest):
        k = STATS.index(kind) if kind in STATS else 0
        if action == "multiply" and lowest:
            if d < planes - 1:
                multiply(kind, d)
        elif action == "multiply":
            pl.when(z + d < planes - 1)(lambda: multiply(kind, d))
        elif action == "wait" and kind[0] == "P":
            receive_all((3 if kind == "P0" else 1) * bars, recv.at[recvs[kind, d]])
        elif action == "wait" and (kind, d) in (("XA", 0), ("YA", 0), ("ZA", 1)):
            block = slot(z + d, ny if k == 1 else y, nx if k == 0 else x, core)
            if lowest or kind == "ZA":
                convert(k, block)
            else:
                pl.when(z < low)(lambda: convert(k, block))
                pl.when(z >= low)(lambda: copy(kind, d, True, lambda end: end.wait_recv()))
        elif action == "wait":
            copy(kind, d, True, lambda end: end.wait_recv())
        elif d == 0 and kind in STATS:
            if lowest or kind == "ZA":
                early(k, stats, (deepest, 8)).start()
            else:
                pl.when(z < low)(lambda: early(k, stats, (deepest, 8)).start())
                pl.when(z >= low)(lambda: copy(kind, d, False, lambda end: end.start()))
        else:
            copy(kind, d, False, lambda end: end.start())

    def carry_out(actions, lowest):
        transposed = False
        while actions:
            name, d = key = group(*actions[0])
            count = 1
            while count < len(actions) and group(*actions[count]) == key:
                count += 1
            batch, actions = actions[:count], actions[count:]

            def run(batch=batch):
                for action in batch:
                    act(*action, lowest)

            if not transposed and batch[0][0] != "start":
                zt[...] = gath[own].T
                transposed = True
            if lowest or d == 0:
                run()
            else:
                pl.when(z + d < planes)(run)

    pl.when(z == 0)(lambda: carry_out(plan(planes, True), True))
    if planes > 1:
        pl.when(z > 0)(lambda: carry_out(plan(planes, False), False))

    def finish(plane):
        counts = [0, 0]
        for action, kind, d in plan(planes, plane == 0):
            raw_sent = d == 0 and (kind == "ZA" or kind in STATS and plane < low)
            if action == "start" and plane + d < planes and not raw_sent:
                for c in range(2):
                    counts[c] += piece(kind, d, False, highs[c])[2][1]
        for c in range(2):
            pl.when(core == c)(lambda c=c: drain(counts[c], send.at[0]))
        raw_rows = (4 * (early_rows + 8) if plane < low else 0) + (2 * (down_depth(bars) + 8) if plane else 0)
        drain(raw_rows, send.at[1])
        part_wait(8 * low - (plane < low) + (planes - low if plane == low - 1 else 0)).wait_send()

    for plane in range(planes):
        pl.when(z == plane)(functools.partial(finish, plane))


def finish_kernel(early_ref, gath, zt, out_hbm, late_ref, sem):
    blocks, _, width = gath.shape
    own = lax.axis_index("blk") * 2 + lax.axis_index("grp")
    ready = width * (blocks - 8)
    copies = [pltpu.make_async_copy(early_ref, out_hbm.at[:, pl.ds(0, ready)], sem.at[0])]
    copies[0].start()
    for i in range(8):
        block = blocks - 8 + i
        product = jnp.dot(zt[...], gath[block], preferred_element_type=jnp.float32).astype(jnp.bfloat16)
        late_ref[:, width * i : width * (i + 1)] = jnp.where(block >= own, product, jnp.bfloat16(0.0))
        if i % 4 == 3:
            at = pl.ds(width * (i - 3), 4 * width)
            to = pl.ds(ready + width * (i - 3), 4 * width)
            copies.append(pltpu.make_async_copy(late_ref.at[:, at], out_hbm.at[:, to], sem.at[len(copies)]))
            copies[-1].start()
    for copy in copies:
        copy.wait()


def shards(planes, returns):
    bars, width = returns.shape
    blocks = planes * 8
    held = blocks * width * (2 * bars + 2 * width) + 6 * bars * width
    vmem = pl.BlockSpec(memory_space=pltpu.VMEM)
    products, gathered, transposed = pl.pallas_call(
        functools.partial(kernel, planes),
        out_shape=[
            jax.ShapeDtypeStruct((width, (blocks - 8) * width), jnp.bfloat16),
            jax.ShapeDtypeStruct((blocks, bars, width), jnp.bfloat16),
            jax.ShapeDtypeStruct((width, bars), jnp.bfloat16),
        ],
        in_specs=[pl.BlockSpec(memory_space=pltpu.HBM)],
        out_specs=[vmem, vmem, vmem],
        scratch_shapes=[
            pltpu.VMEM((bars, width), jnp.float32),
            pltpu.VMEM((blocks, 1, bars), jnp.float32),
            pltpu.VMEM((1, bars), jnp.float32),
            pltpu.VMEM((bars, 128), jnp.float32),
            pltpu.VMEM((3, max(early_depth(bars), down_depth(bars)) + 8, width), jnp.float32),
            pltpu.VMEM((8, width), jnp.float32),
            pltpu.SemaphoreType.DMA,
            pltpu.SemaphoreType.DMA,
            pltpu.SemaphoreType.DMA,
            pltpu.SemaphoreType.DMA((2,)),
            pltpu.SemaphoreType.DMA((14 * planes - 4,)),
        ],
        compiler_params=pltpu.CompilerParams(
            collective_id=0, has_side_effects=True, vmem_limit_bytes=held + 4 * 1024 * 1024
        ),
    )(pltpu.with_memory_space_constraint(returns, pltpu.HBM))
    return pl.pallas_call(
        finish_kernel,
        out_shape=jax.ShapeDtypeStruct((width, blocks * width), jnp.bfloat16),
        in_specs=[vmem, vmem, vmem],
        out_specs=pl.BlockSpec(memory_space=pltpu.HBM),
        scratch_shapes=[pltpu.VMEM((width, 8 * width), jnp.bfloat16), pltpu.SemaphoreType.DMA((3,))],
        compiler_params=pltpu.CompilerParams(vmem_limit_bytes=4 * 1024 * 1024),
    )(*(pltpu.with_memory_space_constraint(a, pltpu.VMEM) for a in (products, gathered, transposed)))


def solution(mesh):
    planes = mesh.shape["blk"] // 4
    in_specs = (P(None, ("blk", "grp")),)
    out_specs = P(("blk", "grp"), None)
    return jax.shard_map(
        functools.partial(shards, planes), mesh=mesh, in_specs=in_specs, out_specs=out_specs, check_vma=False
    )
```

```python
import functools
import math

import jax
import jax.numpy as jnp
from jax import lax
from jax.experimental import pallas as pl
from jax.experimental.pallas import tpu as pltpu
from jax.sharding import PartitionSpec as P

MESH = pl.DeviceIdType.MESH
DOWN = ("ZA", "ZB", "ZO", "ZX", "ZY", "ZD")
SPREAD = ("XA", "XB", "YA", "YB", "D0", "D1")
REST = ("XR", "YR")
PARTNER = ("P0", "P1", "P2", "P3", "P4", "P5")
KINDS = DOWN + SPREAD + REST
STATS = ("XA", "YA", "ZA")
HIGHS = (24, 26)
WAITS_LOW = (
    {
        "XA": 0, "YA": 1, "YB": 3, "YR": 4, "XB": 6, "XR": 7, "D0": 9, "D1": 11,
        "M0": 24, "M1": 27,
    },
    {
        "ZA": 2, "ZO": 5, "ZB": 8, "XA": 12, "YB": 13, "XB": 15, "D0": 18, "YA": 20,
        "ZY": 21, "ZX": 22, "M0": 37, "D1": 40, "ZD": 42, "M1": 49,
    },
    {
        "ZA": 10, "ZB": 14, "YA": 17, "ZO": 23, "XA": 25, "YB": 26, "ZY": 29, "XB": 31,
        "ZX": 38, "D0": 39, "D1": 41, "ZD": 44, "M0": 45, "M1": 50,
    },
    {
        "ZA": 16, "ZB": 19, "ZO": 28, "ZY": 30, "XA": 32, "YA": 33, "YB": 34, "XB": 35,
        "ZX": 36, "M0": 43, "D0": 46, "D1": 47, "ZD": 48, "M1": 51,
    },
)
WAITS_HIGH = (
    {
        "XR": 2, "YB": 3, "YR": 5, "XA": 9, "D1": 17, "D0": 19, "YA": 21, "XB": 26,
        "M0": 27, "M1": 28,
    },
    {
        "ZA": 0, "ZB": 1, "ZO": 7, "ZY": 10, "XA": 12, "XB": 13, "ZX": 16, "ZD": 18,
        "YB": 20, "D0": 25, "YA": 33, "D1": 34, "M0": 36, "M1": 37,
    },
    {
        "ZA": 4, "ZB": 6, "ZO": 8, "ZY": 11, "YA": 14, "ZX": 15, "ZD": 22, "YB": 23,
        "XB": 24, "XA": 29, "D1": 30, "D0": 31, "M0": 32, "M1": 35,
    },
)
PERIOD = 16
SENDS_LOW = (
    "P5", "D0", "YR", "D1", "ZD", "YA", "ZX", "ZY", "P4", "P0",
    "XA", "P3", "ZO", "XR", "ZA", "ZB", "YB", "P1", "XB", "P2",
)
SENDS_HIGH = (
    "P5", "ZX", "D0", "ZY", "XR", "ZA", "P1", "ZB", "XB", "ZO",
    "YR", "P3", "ZD", "D1", "YB", "P2", "P0", "P4", "XA", "YA",
)

def needs(kind, d):
    first = d == 0
    return {
        "ZA": [] if first else ["ZA"],
        "ZB": [] if first else ["ZA", "ZB"],
        "ZO": [] if first else ["ZO"],
        "ZX": ["XR"] if first else ["ZX"],
        "ZY": ["YR"] if first else ["ZY"],
        "ZD": ["D1"] if first else ["ZD"],
        "XA": [] if first else ["ZA"],
        "YA": [] if first else ["ZA"],
        "XB": [] if first else ["ZA", "ZB"],
        "YB": [] if first else ["ZA", "ZB"],
        "XR": [],
        "YR": [],
        "D0": ["XA"],
        "D1": ["YB", "YR"] if first else ["YB"],
        "P0": [] if first else ["ZA", "ZB", "ZO"],
        "P1": ["XA", "XB", "XR" if first else "ZX"],
        "P2": ["YA", "YB", "YR" if first else "ZY"],
        "P3": ["D0"],
        "P4": ["D1"],
        "P5": ["ZD"],
    }[kind]


def early_depth(bars):
    return bars * 14 // 32 // 16 * 16


def early_depth(bars):
    return bars * 14 // 32 // 16 * 16


def down_depth(bars):
    return bars * 15 // 32 // 16 * 16


def group(action, kind, d):
    if action == "start" and kind in DOWN:
        return ("sends down", d)
    return ("holds", d)


def plan(planes, lowest):
    waits, sends = (WAITS_LOW, SENDS_LOW) if lowest else (WAITS_HIGH, SENDS_HIGH)
    span = planes if lowest else planes - 1
    events = []
    for d in range(span):
        kinds = SPREAD + (DOWN if d else REST) + ("M0", "M1")
        known = min(d, len(waits) - 1)
        events += [(waits[known][kind] + PERIOD * (d - known), kind, d) for kind in kinds]
    here, sent, actions = set(), set(), []

    def send():
        for d in range(span):
            for kind in sends:
                absent = (kind in REST and d > 0) or (kind in DOWN and lowest) or (kind == "P5" and d == 0)
                if (kind, d) not in sent and not absent and all((k, d) in here for k in needs(kind, d)):
                    sent.add((kind, d))
                    actions.append(("start", kind, d))

    for kind in STATS[:2] if lowest else STATS:
        sent.add((kind, 0))
        actions.append(("start", kind, 0))
    send()
    products = []

    def multiply_all():
        actions.extend(("wait", "P" + kind[1], d) for kind, d in products)
        actions.extend(("multiply", kind, d) for kind, d in products)
        products.clear()

    for _, kind, d in sorted(events):
        if kind in ("M0", "M1"):
            if not lowest or d == planes - 1:
                multiply_all()
            products.append((kind, d))
            if not lowest or d == planes - 1:
                multiply_all()
        else:
            multiply_all()
            actions.append(("wait", kind, d))
            here.add((kind, d))
            send()
    multiply_all()
    return actions


def kernel(
    planes, r_hbm, out_ref, gath, zt, r_ref, parts, total, market, raw, stats, landed, load_sem, psend, precv, send, recv
):
    bars, width = r_ref.shape
    blocks = gath.shape[0]
    low = min(2, planes)
    blk, core = lax.axis_index("blk"), lax.axis_index("grp")
    x, y, z = lax.rem(blk, 2), lax.rem(lax.div(blk, 2), 2), lax.div(blk, 4)
    nx, ny, nc = 1 - x, 1 - y, 1 - core
    highs = tuple(bars * n // 32 // 16 * 16 for n in HIGHS)
    half = bars * 13 // 32 // 16 * 16
    early_rows = early_depth(bars)

    def device(zz, yy, xx, cc):
        return {"blk": (zz * 2 + yy) * 2 + xx, "grp": cc}

    def slot(zz, yy, xx, cc):
        return ((zz * 2 + yy) * 2 + xx) * 2 + cc

    own = slot(z, y, x, core)
    load = pltpu.make_async_copy(r_hbm, r_ref, load_sem)
    load.start()
    barrier = pltpu.get_barrier_semaphore()

    def greet(target):
        pl.semaphore_signal(barrier, inc=1, device_id=target, device_id_type=MESH)

    @pl.when(z < low)
    def _():
        for j in range(blocks):
            pl.when(own != j)(functools.partial(greet, {"blk": j // 2, "grp": j % 2}))

    if planes > low + 1:

        @pl.when(jnp.logical_and(z >= low, z < planes - 1))
        def _():
            greet(device(z + 1, y, x, core))

    load.wait()
    lanes = r_ref[:, :128]
    for i in range(1, width // 128):
        lanes = lanes + r_ref[:, 128 * i : 128 * (i + 1)]
    parts[own] = jnp.sum(lanes.T, axis=0, keepdims=True)

    def part_copy(target):
        return pltpu.make_async_remote_copy(
            parts.at[own], parts.at[own], psend, precv, device_id=target, device_id_type=MESH
        )

    def part_wait(count):
        rest = parts.at[pl.ds(0, count)]
        return pltpu.make_async_remote_copy(
            rest, rest, psend, precv, device_id=device(z, y, x, nc), device_id_type=MESH
        )

    def total_copy(zz):
        return pltpu.make_async_remote_copy(
            total, total, psend, precv, device_id=device(zz, y, x, core), device_id_type=MESH
        )

    pl.semaphore_wait(barrier, 8 * low + jnp.where(z < low, -1, 0) + jnp.where(z > low, 1, 0))
    for j in range(8 * low):
        pl.when(own != j)(lambda j=j: part_copy({"blk": j // 2, "grp": j % 2}).start())

    recvs = {}
    for d in range(planes):
        for kind in SPREAD + (DOWN if d else REST) + ("P0", "P1"):
            recvs[kind, d] = len(recvs)

    def early(k, source, target_ref):
        kind, d, target = (
            ("XA", 0, device(z, y, nx, core)),
            ("YA", 0, device(z, ny, x, core)),
            ("ZA", 1, device(z - 1, y, x, core)),
        )[k]
        return pltpu.make_async_remote_copy(
            source,
            target_ref,
            send.at[1],
            recv.at[recvs[kind, d]],
            device_id=target,
            device_id_type=MESH,
        )

    depths = (early_rows, early_rows, down_depth(bars))
    stat_rows = stats.shape[0]

    def early_raw(k):
        rows = pl.ds(0, depths[k])
        early(k, r_ref.at[rows], raw.at[k, rows]).start()

    @pl.when(z < low)
    def _():
        early_raw(0)
        early_raw(1)

    if planes > 1:
        pl.when(z > 0)(lambda: early_raw(2))

    @pl.loop(0, z * 8)
    def _(block):
        at = pl.ds(pl.multiple_of(block * width, width), width)
        out_ref[:, at] = jnp.zeros((width, width), jnp.bfloat16)

    @pl.when(z < low)
    def _():
        part_wait(blocks - 1).wait_recv()
        total[...] = jnp.sum(parts[...], axis=0) * (1.0 / (width * blocks))

    if planes > low:

        @pl.when(z == low - 1)
        def _():
            for zz in range(low, planes):
                total_copy(zz).start()

        pl.when(z >= low)(lambda: total_copy(z).wait_recv())

    market[...] = jnp.broadcast_to(total[...], (128, bars)).T
    first = lax.broadcasted_iota(jnp.int32, (stat_rows, 128), 0) == 0
    for i in range(width // 128):
        at = slice(128 * i, 128 * (i + 1))
        excess = r_ref[:, at] - market[...]
        mean = jnp.mean(excess, axis=0, keepdims=True)
        deviation = excess - mean
        inverse = lax.rsqrt(jnp.mean(deviation * deviation, axis=0, keepdims=True) + 1e-06) / math.sqrt(bars)
        stats[:, at] = jnp.where(first, mean, inverse)
        gath[own, :, at] = (deviation * inverse).astype(jnp.bfloat16)

    def convert(k, block):
        depth = depths[k]
        receive_all(2 * (depth + stat_rows), recv.at[recvs[("XA", "YA", "ZA")[k], k // 2]])
        for i in range(width // 128):
            at = slice(128 * i, 128 * (i + 1))
            deviation = raw[k, :depth, at] - market[:depth] - landed[k, :1, at]
            gath[block, :depth, at] = (deviation * landed[k, 1:2, at]).astype(jnp.bfloat16)

    def piece(kind, d, arriving, high):
        link = kind[0] if kind[0] != "D" else ("Y" if kind == "D0" else "X")
        first = half
        if link == "Z" and d == int(arriving):
            first = down_depth(bars)
        elif link != "Z" and d == 0:
            first = early_rows
        rows_a, rows_b, rows_r = (0, first), (first, high - first), (high, bars - high)
        if arriving:
            flip = {"X": (0, 1), "Y": (1, 0), "D": (1, 1)}.get(kind[0], (0, 0))
        else:
            flip = {"D0": (0, 1), "D1": (1, 0)}.get(kind, (0, 0))
        if link == "Z":
            flip = {"ZX": (0, 1), "ZY": (1, 0), "ZD": (1, 1)}.get(kind, (0, 0))
            rows = {"ZA": rows_a, "ZB": rows_b}.get(kind, rows_r)
        elif link == "P":
            flip = {"P0": (0, 0), "P1": (0, 1), "P2": (1, 0)}.get(kind, (1, 1))
            rows = {"P3": rows_a, "P4": rows_b if d else (first, bars - first), "P5": rows_r}.get(kind, (0, bars))
        else:
            last = (first, bars - first) if d == 0 else rows_b
            rows = {"A": rows_a, "B": rows_b, "R": rows_r, "0": rows_a, "1": last}[kind[1]]
        return link, flip, rows

    def copy(kind, d, arriving, run):
        if piece(kind, d, arriving, highs[0]) == piece(kind, d, arriving, highs[1]):
            run(core_copy(kind, d, arriving, highs[0]))
        else:
            for c in range(2):
                pl.when(core == c)(lambda c=c: run(core_copy(kind, d, arriving, highs[c])))

    def core_copy(kind, d, arriving, high):
        link, flip, rows = piece(kind, d, arriving, high)
        down = link == "Z"
        block = slot(z + d, ny if flip[0] else y, nx if flip[1] else x, core)
        target = {
            "Z": device(z - 1, y, x, core),
            "X": device(z, y, nx, core),
            "Y": device(z, ny, x, core),
            "P": device(z, y, x, nc),
        }[link]
        ref = gath.at[block, pl.ds(*rows)]
        if link == "P":
            kind = "P0" if kind in PARTNER[:3] else "P1"
        return pltpu.make_async_remote_copy(
            ref,
            ref,
            send.at[0],
            recv.at[recvs[kind, d + 1 if down and not arriving else d]],
            device_id=target,
            device_id_type=MESH,
        )

    def multiply(kind, d):
        base, count = (0, 6) if kind == "M0" else (6, 2)

        for i in range(base, base + count):
            block = slot(z + d, ny if i & 4 else y, nx if i & 2 else x, i & 1)
            at = pl.ds(pl.multiple_of(block * width, width), width)
            product = jnp.dot(zt[...], gath[block], preferred_element_type=jnp.float32).astype(jnp.bfloat16)
            if d == 0:
                product = jnp.where(block >= own, product, jnp.bfloat16(0.0))
            out_ref[:, at] = product

    def whole(count, sem):
        sizes = [n for n in range(8, bars + 1, 8)]
        fits = lambda rows_in_all: [n for n in sizes if rows_in_all % n == 0 and rows_in_all // n <= blocks]
        extra = next(n for n in [0, *sizes] if fits(count - n))
        parts_of = [(count - extra, fits(count - extra)[-1])] + ([(extra, extra)] if extra else [])
        refs = [gath.at[pl.ds(0, number // rows), pl.ds(0, rows)] for number, rows in parts_of]
        partner = device(z, y, x, nc)
        return [
            pltpu.make_async_remote_copy(ref, ref, sem, sem, device_id=partner, device_id_type=MESH) for ref in refs
        ]

    def receive_all(count, sem):
        for part in whole(count, sem):
            part.wait_recv()

    def drain(count, sem):
        for part in whole(count, sem):
            part.wait_send()

    def act(action, kind, d, lowest):
        k = STATS.index(kind) if kind in STATS else 0
        if action == "multiply" and lowest:
            if d < planes - 1:
                multiply(kind, d)
        elif action == "multiply":
            pl.when(z + d < planes - 1)(lambda: multiply(kind, d))
        elif action == "wait" and kind[0] == "P":
            receive_all((3 if kind == "P0" else 1) * bars, recv.at[recvs[kind, d]])
        elif action == "wait" and (kind, d) in (("XA", 0), ("YA", 0), ("ZA", 1)):
            block = slot(z + d, ny if k == 1 else y, nx if k == 0 else x, core)
            if lowest or kind == "ZA":
                convert(k, block)
            else:
                pl.when(z < low)(lambda: convert(k, block))
                pl.when(z >= low)(lambda: copy(kind, d, True, lambda end: end.wait_recv()))
        elif action == "wait":
            copy(kind, d, True, lambda end: end.wait_recv())
        elif d == 0 and kind in STATS:
            if lowest or kind == "ZA":
                early(k, stats, landed.at[k]).start()
            else:
                pl.when(z < low)(lambda: early(k, stats, landed.at[k]).start())
                pl.when(z >= low)(lambda: copy(kind, d, False, lambda end: end.start()))
        else:
            copy(kind, d, False, lambda end: end.start())

    def carry_out(actions, lowest):
        transposed = False
        while actions:
            name, d = key = group(*actions[0])
            count = 1
            while count < len(actions) and group(*actions[count]) == key:
                count += 1
            batch, actions = actions[:count], actions[count:]

            def run(batch=batch):
                for action in batch:
                    act(*action, lowest)

            if not transposed and batch[0][0] != "start":
                zt[...] = gath[own].T
                transposed = True
            if lowest or d == 0:
                run()
            else:
                pl.when(z + d < planes)(run)

    pl.when(z == 0)(lambda: carry_out(plan(planes, True), True))
    if planes > 1:
        pl.when(z > 0)(lambda: carry_out(plan(planes, False), False))

    def finish(plane):
        counts = [0, 0]
        for action, kind, d in plan(planes, plane == 0):
            raw_sent = d == 0 and (kind == "ZA" or kind in STATS and plane < low)
            if action == "start" and plane + d < planes and not raw_sent:
                for c in range(2):
                    counts[c] += piece(kind, d, False, highs[c])[2][1]
        for c in range(2):
            pl.when(core == c)(lambda c=c: drain(counts[c], send.at[0]))
        raw_rows = (4 * (early_rows + stat_rows) if plane < low else 0) + (
            2 * (down_depth(bars) + stat_rows) if plane else 0
        )
        drain(raw_rows, send.at[1])
        part_wait(8 * low - (plane < low) + (planes - low if plane == low - 1 else 0)).wait_send()

    for plane in range(planes):
        pl.when(z == plane)(functools.partial(finish, plane))


def finish_kernel(early_ref, gath, zt, out_hbm, late_ref, sem):
    blocks, _, width = gath.shape
    own = lax.axis_index("blk") * 2 + lax.axis_index("grp")
    ready = width * (blocks - 8)
    copies = [pltpu.make_async_copy(early_ref, out_hbm.at[:, pl.ds(0, ready)], sem.at[0])]
    copies[0].start()
    for i in range(8):
        block = blocks - 8 + i
        product = jnp.dot(zt[...], gath[block], preferred_element_type=jnp.float32).astype(jnp.bfloat16)
        late_ref[:, width * i : width * (i + 1)] = jnp.where(block >= own, product, jnp.bfloat16(0.0))
        if i % 4 == 3:
            at = pl.ds(width * (i - 3), 4 * width)
            to = pl.ds(ready + width * (i - 3), 4 * width)
            copies.append(pltpu.make_async_copy(late_ref.at[:, at], out_hbm.at[:, to], sem.at[len(copies)]))
            copies[-1].start()
    for copy in copies:
        copy.wait()


def shards(planes, returns):
    bars, width = returns.shape
    blocks = planes * 8
    held = blocks * width * (2 * bars + 2 * width) + 6 * bars * width
    vmem = pl.BlockSpec(memory_space=pltpu.VMEM)
    products, gathered, transposed = pl.pallas_call(
        functools.partial(kernel, planes),
        out_shape=[
            jax.ShapeDtypeStruct((width, (blocks - 8) * width), jnp.bfloat16),
            jax.ShapeDtypeStruct((blocks, bars, width), jnp.bfloat16),
            jax.ShapeDtypeStruct((width, bars), jnp.bfloat16),
        ],
        in_specs=[pl.BlockSpec(memory_space=pltpu.HBM)],
        out_specs=[vmem, vmem, vmem],
        scratch_shapes=[
            pltpu.VMEM((bars, width), jnp.float32),
            pltpu.VMEM((blocks, 1, bars), jnp.float32),
            pltpu.VMEM((1, bars), jnp.float32),
            pltpu.VMEM((bars, 128), jnp.float32),
            pltpu.VMEM((3, max(early_depth(bars), down_depth(bars)), width), jnp.float32),
            pltpu.VMEM((4, width), jnp.float32),
            pltpu.VMEM((3, 4, width), jnp.float32),
            pltpu.SemaphoreType.DMA,
            pltpu.SemaphoreType.DMA,
            pltpu.SemaphoreType.DMA,
            pltpu.SemaphoreType.DMA((2,)),
            pltpu.SemaphoreType.DMA((14 * planes - 4,)),
        ],
        compiler_params=pltpu.CompilerParams(
            collective_id=0, has_side_effects=True, vmem_limit_bytes=held + 4 * 1024 * 1024
        ),
    )(pltpu.with_memory_space_constraint(returns, pltpu.HBM))
    return pl.pallas_call(
        finish_kernel,
        out_shape=jax.ShapeDtypeStruct((width, blocks * width), jnp.bfloat16),
        in_specs=[vmem, vmem, vmem],
        out_specs=pl.BlockSpec(memory_space=pltpu.HBM),
        scratch_shapes=[pltpu.VMEM((width, 8 * width), jnp.bfloat16), pltpu.SemaphoreType.DMA((3,))],
        compiler_params=pltpu.CompilerParams(vmem_limit_bytes=4 * 1024 * 1024),
    )(*(pltpu.with_memory_space_constraint(a, pltpu.VMEM) for a in (products, gathered, transposed)))


def solution(mesh):
    planes = mesh.shape["blk"] // 4
    in_specs = (P(None, ("blk", "grp")),)
    out_specs = P(("blk", "grp"), None)
    return jax.shard_map(
        functools.partial(shards, planes), mesh=mesh, in_specs=in_specs, out_specs=out_specs, check_vma=False
    )
```

```python
import functools
import math

import jax
import jax.numpy as jnp
from jax import lax
from jax.experimental import pallas as pl
from jax.experimental.pallas import tpu as pltpu
from jax.sharding import PartitionSpec as P

MESH = pl.DeviceIdType.MESH
DOWN = ("ZA", "ZB", "ZO", "ZX", "ZY", "ZD")
SPREAD = ("XA", "XB", "YA", "YB", "D0", "D1")
REST = ("XR", "YR")
PARTNER = ("P0", "P1", "P2", "P3", "P4", "P5")
KINDS = DOWN + SPREAD + REST
STATS = ("XA", "YA", "ZA")
HIGHS = (24, 26)
WAITS_LOW = (
    {
        "XA": 0, "YA": 1, "YB": 3, "YR": 4, "XB": 6, "XR": 7, "D0": 9, "D1": 11,
        "M0": 24, "M1": 27,
    },
    {
        "ZA": 2, "ZO": 5, "ZB": 8, "XA": 12, "YB": 13, "XB": 15, "D0": 18, "YA": 20,
        "ZY": 21, "ZX": 22, "M0": 37, "D1": 40, "ZD": 42, "M1": 49,
    },
    {
        "ZA": 10, "ZB": 14, "YA": 17, "ZO": 23, "XA": 25, "YB": 26, "ZY": 29, "XB": 31,
        "ZX": 38, "D0": 39, "D1": 41, "ZD": 44, "M0": 45, "M1": 50,
    },
    {
        "ZA": 16, "ZB": 19, "ZO": 28, "ZY": 30, "XA": 32, "YA": 33, "YB": 34, "XB": 35,
        "ZX": 36, "M0": 43, "D0": 46, "D1": 47, "ZD": 48, "M1": 51,
    },
)
WAITS_HIGH = (
    {
        "XR": 2, "YB": 3, "YR": 5, "XA": 9, "D1": 17, "D0": 19, "YA": 21, "XB": 26,
        "M0": 27, "M1": 28,
    },
    {
        "ZA": 0, "ZB": 1, "ZO": 7, "ZY": 10, "XA": 12, "XB": 13, "ZX": 16, "ZD": 18,
        "YB": 20, "D0": 25, "YA": 33, "D1": 34, "M0": 36, "M1": 37,
    },
    {
        "ZA": 4, "ZB": 6, "ZO": 8, "ZY": 11, "YA": 14, "ZX": 15, "ZD": 22, "YB": 23,
        "XB": 24, "XA": 29, "D1": 30, "D0": 31, "M0": 32, "M1": 35,
    },
)
PERIOD = 16
SENDS_LOW = (
    "P5", "D0", "YR", "D1", "ZD", "YA", "ZX", "ZY", "P4", "P0",
    "XA", "P3", "ZO", "XR", "ZA", "ZB", "YB", "P1", "XB", "P2",
)
SENDS_HIGH = (
    "P5", "ZX", "D0", "ZY", "XR", "ZA", "P1", "ZB", "XB", "ZO",
    "YR", "P3", "ZD", "D1", "YB", "P2", "P0", "P4", "XA", "YA",
)

def needs(kind, d):
    first = d == 0
    return {
        "ZA": [] if first else ["ZA"],
        "ZB": [] if first else ["ZA", "ZB"],
        "ZO": [] if first else ["ZO"],
        "ZX": ["XR"] if first else ["ZX"],
        "ZY": ["YR"] if first else ["ZY"],
        "ZD": ["D1"] if first else ["ZD"],
        "XA": [] if first else ["ZA"],
        "YA": [] if first else ["ZA"],
        "XB": [] if first else ["ZA", "ZB"],
        "YB": [] if first else ["ZA", "ZB"],
        "XR": [],
        "YR": [],
        "D0": ["XA"],
        "D1": ["YB", "YR"] if first else ["YB"],
        "P0": [] if first else ["ZA", "ZB", "ZO"],
        "P1": ["XA", "XB", "XR" if first else "ZX"],
        "P2": ["YA", "YB", "YR" if first else "ZY"],
        "P3": ["D0"],
        "P4": ["D1"],
        "P5": ["ZD"],
    }[kind]


def early_depth(bars):
    return bars * 15 // 32 // 16 * 16


def early_depth(bars):
    return bars * 15 // 32 // 16 * 16


def down_depth(bars):
    return bars * 16 // 32 // 16 * 16


def group(action, kind, d):
    if action == "start" and kind in DOWN:
        return ("sends down", d)
    return ("holds", d)


def plan(planes, lowest):
    waits, sends = (WAITS_LOW, SENDS_LOW) if lowest else (WAITS_HIGH, SENDS_HIGH)
    span = planes if lowest else planes - 1
    events = []
    for d in range(span):
        kinds = SPREAD + (DOWN if d else REST) + ("M0", "M1")
        known = min(d, len(waits) - 1)
        events += [(waits[known][kind] + PERIOD * (d - known), kind, d) for kind in kinds]
    here, sent, actions = set(), set(), []

    def send():
        for d in range(span):
            for kind in sends:
                absent = (kind in REST and d > 0) or (kind in DOWN and lowest) or (kind == "P5" and d == 0)
                if (kind, d) not in sent and not absent and all((k, d) in here for k in needs(kind, d)):
                    sent.add((kind, d))
                    actions.append(("start", kind, d))

    for kind in STATS[:2] if lowest else STATS:
        sent.add((kind, 0))
        actions.append(("start", kind, 0))
    send()
    products = []

    def multiply_all():
        actions.extend(("wait", "P" + kind[1], d) for kind, d in products)
        actions.extend(("multiply", kind, d) for kind, d in products)
        products.clear()

    for _, kind, d in sorted(events):
        if kind in ("M0", "M1"):
            if not lowest or d == planes - 1:
                multiply_all()
            products.append((kind, d))
            if not lowest or d == planes - 1:
                multiply_all()
        else:
            multiply_all()
            actions.append(("wait", kind, d))
            here.add((kind, d))
            send()
    multiply_all()
    return actions


def kernel(
    planes, r_hbm, out_ref, gath, zt, r_ref, parts, total, market, raw, stats, landed, load_sem, psend, precv, send, recv
):
    bars, width = r_ref.shape
    blocks = gath.shape[0]
    low = min(2, planes)
    blk, core = lax.axis_index("blk"), lax.axis_index("grp")
    x, y, z = lax.rem(blk, 2), lax.rem(lax.div(blk, 2), 2), lax.div(blk, 4)
    nx, ny, nc = 1 - x, 1 - y, 1 - core
    highs = tuple(bars * n // 32 // 16 * 16 for n in HIGHS)
    half = bars * 13 // 32 // 16 * 16
    early_rows = early_depth(bars)

    def device(zz, yy, xx, cc):
        return {"blk": (zz * 2 + yy) * 2 + xx, "grp": cc}

    def slot(zz, yy, xx, cc):
        return ((zz * 2 + yy) * 2 + xx) * 2 + cc

    own = slot(z, y, x, core)
    load = pltpu.make_async_copy(r_hbm, r_ref, load_sem)
    load.start()
    barrier = pltpu.get_barrier_semaphore()

    def greet(target):
        pl.semaphore_signal(barrier, inc=1, device_id=target, device_id_type=MESH)

    @pl.when(z < low)
    def _():
        for j in range(blocks):
            pl.when(own != j)(functools.partial(greet, {"blk": j // 2, "grp": j % 2}))

    if planes > low + 1:

        @pl.when(jnp.logical_and(z >= low, z < planes - 1))
        def _():
            greet(device(z + 1, y, x, core))

    load.wait()
    lanes = r_ref[:, :128]
    for i in range(1, width // 128):
        lanes = lanes + r_ref[:, 128 * i : 128 * (i + 1)]
    parts[own] = jnp.sum(lanes.T, axis=0, keepdims=True)

    def part_copy(target):
        return pltpu.make_async_remote_copy(
            parts.at[own], parts.at[own], psend, precv, device_id=target, device_id_type=MESH
        )

    def part_wait(count):
        rest = parts.at[pl.ds(0, count)]
        return pltpu.make_async_remote_copy(
            rest, rest, psend, precv, device_id=device(z, y, x, nc), device_id_type=MESH
        )

    def total_copy(zz):
        return pltpu.make_async_remote_copy(
            total, total, psend, precv, device_id=device(zz, y, x, core), device_id_type=MESH
        )

    pl.semaphore_wait(barrier, 8 * low + jnp.where(z < low, -1, 0) + jnp.where(z > low, 1, 0))
    for j in range(8 * low):
        pl.when(own != j)(lambda j=j: part_copy({"blk": j // 2, "grp": j % 2}).start())

    recvs = {}
    for d in range(planes):
        for kind in SPREAD + (DOWN if d else REST) + ("P0", "P1"):
            recvs[kind, d] = len(recvs)

    def early(k, source, target_ref):
        kind, d, target = (
            ("XA", 0, device(z, y, nx, core)),
            ("YA", 0, device(z, ny, x, core)),
            ("ZA", 1, device(z - 1, y, x, core)),
        )[k]
        return pltpu.make_async_remote_copy(
            source,
            target_ref,
            send.at[1],
            recv.at[recvs[kind, d]],
            device_id=target,
            device_id_type=MESH,
        )

    depths = (early_rows, early_rows, down_depth(bars))
    stat_rows = stats.shape[0]

    def early_raw(k):
        rows = pl.ds(0, depths[k])
        early(k, r_ref.at[rows], raw.at[k, rows]).start()

    @pl.when(z < low)
    def _():
        early_raw(0)
        early_raw(1)

    if planes > 1:
        pl.when(z > 0)(lambda: early_raw(2))

    @pl.loop(0, z * 8)
    def _(block):
        at = pl.ds(pl.multiple_of(block * width, width), width)
        out_ref[:, at] = jnp.zeros((width, width), jnp.bfloat16)

    @pl.when(z < low)
    def _():
        part_wait(blocks - 1).wait_recv()
        total[...] = jnp.sum(parts[...], axis=0) * (1.0 / (width * blocks))

    if planes > low:

        @pl.when(z == low - 1)
        def _():
            for zz in range(low, planes):
                total_copy(zz).start()

        pl.when(z >= low)(lambda: total_copy(z).wait_recv())

    market[...] = jnp.broadcast_to(total[...], (128, bars)).T
    first = lax.broadcasted_iota(jnp.int32, (stat_rows, 128), 0) == 0
    for i in range(width // 128):
        at = slice(128 * i, 128 * (i + 1))
        excess = r_ref[:, at] - market[...]
        mean = jnp.mean(excess, axis=0, keepdims=True)
        deviation = excess - mean
        inverse = lax.rsqrt(jnp.mean(deviation * deviation, axis=0, keepdims=True) + 1e-06) / math.sqrt(bars)
        stats[:, at] = jnp.where(first, mean, inverse)
        gath[own, :, at] = (deviation * inverse).astype(jnp.bfloat16)

    def convert(k, block):
        depth = depths[k]
        receive_all(2 * (depth + stat_rows), recv.at[recvs[("XA", "YA", "ZA")[k], k // 2]])
        for i in range(width // 128):
            at = slice(128 * i, 128 * (i + 1))
            deviation = raw[k, :depth, at] - market[:depth] - landed[k, :1, at]
            gath[block, :depth, at] = (deviation * landed[k, 1:2, at]).astype(jnp.bfloat16)

    def piece(kind, d, arriving, high):
        link = kind[0] if kind[0] != "D" else ("Y" if kind == "D0" else "X")
        first = half
        if link == "Z" and d == int(arriving):
            first = down_depth(bars)
        elif link != "Z" and d == 0:
            first = early_rows
        rows_a, rows_b, rows_r = (0, first), (first, high - first), (high, bars - high)
        if arriving:
            flip = {"X": (0, 1), "Y": (1, 0), "D": (1, 1)}.get(kind[0], (0, 0))
        else:
            flip = {"D0": (0, 1), "D1": (1, 0)}.get(kind, (0, 0))
        if link == "Z":
            flip = {"ZX": (0, 1), "ZY": (1, 0), "ZD": (1, 1)}.get(kind, (0, 0))
            rows = {"ZA": rows_a, "ZB": rows_b}.get(kind, rows_r)
        elif link == "P":
            flip = {"P0": (0, 0), "P1": (0, 1), "P2": (1, 0)}.get(kind, (1, 1))
            rows = {"P3": rows_a, "P4": rows_b if d else (first, bars - first), "P5": rows_r}.get(kind, (0, bars))
        else:
            last = (first, bars - first) if d == 0 else rows_b
            rows = {"A": rows_a, "B": rows_b, "R": rows_r, "0": rows_a, "1": last}[kind[1]]
        return link, flip, rows

    def copy(kind, d, arriving, run):
        if piece(kind, d, arriving, highs[0]) == piece(kind, d, arriving, highs[1]):
            run(core_copy(kind, d, arriving, highs[0]))
        else:
            for c in range(2):
                pl.when(core == c)(lambda c=c: run(core_copy(kind, d, arriving, highs[c])))

    def core_copy(kind, d, arriving, high):
        link, flip, rows = piece(kind, d, arriving, high)
        down = link == "Z"
        block = slot(z + d, ny if flip[0] else y, nx if flip[1] else x, core)
        target = {
            "Z": device(z - 1, y, x, core),
            "X": device(z, y, nx, core),
            "Y": device(z, ny, x, core),
            "P": device(z, y, x, nc),
        }[link]
        ref = gath.at[block, pl.ds(*rows)]
        if link == "P":
            kind = "P0" if kind in PARTNER[:3] else "P1"
        return pltpu.make_async_remote_copy(
            ref,
            ref,
            send.at[0],
            recv.at[recvs[kind, d + 1 if down and not arriving else d]],
            device_id=target,
            device_id_type=MESH,
        )

    def multiply(kind, d):
        base, count = (0, 6) if kind == "M0" else (6, 2)

        for i in range(base, base + count):
            block = slot(z + d, ny if i & 4 else y, nx if i & 2 else x, i & 1)
            at = pl.ds(pl.multiple_of(block * width, width), width)
            product = jnp.dot(zt[...], gath[block], preferred_element_type=jnp.float32).astype(jnp.bfloat16)
            if d == 0:
                product = jnp.where(block >= own, product, jnp.bfloat16(0.0))
            out_ref[:, at] = product

    def whole(count, sem):
        sizes = [n for n in range(8, bars + 1, 8)]
        fits = lambda rows_in_all: [n for n in sizes if rows_in_all % n == 0 and rows_in_all // n <= blocks]
        extra = next(n for n in [0, *sizes] if fits(count - n))
        parts_of = [(count - extra, fits(count - extra)[-1])] + ([(extra, extra)] if extra else [])
        refs = [gath.at[pl.ds(0, number // rows), pl.ds(0, rows)] for number, rows in parts_of]
        partner = device(z, y, x, nc)
        return [
            pltpu.make_async_remote_copy(ref, ref, sem, sem, device_id=partner, device_id_type=MESH) for ref in refs
        ]

    def receive_all(count, sem):
        for part in whole(count, sem):
            part.wait_recv()

    def drain(count, sem):
        for part in whole(count, sem):
            part.wait_send()

    def act(action, kind, d, lowest):
        k = STATS.index(kind) if kind in STATS else 0
        if action == "multiply" and lowest:
            if d < planes - 1:
                multiply(kind, d)
        elif action == "multiply":
            pl.when(z + d < planes - 1)(lambda: multiply(kind, d))
        elif action == "wait" and kind[0] == "P":
            receive_all((3 if kind == "P0" else 1) * bars, recv.at[recvs[kind, d]])
        elif action == "wait" and (kind, d) in (("XA", 0), ("YA", 0), ("ZA", 1)):
            block = slot(z + d, ny if k == 1 else y, nx if k == 0 else x, core)
            if lowest or kind == "ZA":
                convert(k, block)
            else:
                pl.when(z < low)(lambda: convert(k, block))
                pl.when(z >= low)(lambda: copy(kind, d, True, lambda end: end.wait_recv()))
        elif action == "wait":
            copy(kind, d, True, lambda end: end.wait_recv())
        elif d == 0 and kind in STATS:
            if lowest or kind == "ZA":
                early(k, stats, landed.at[k]).start()
            else:
                pl.when(z < low)(lambda: early(k, stats, landed.at[k]).start())
                pl.when(z >= low)(lambda: copy(kind, d, False, lambda end: end.start()))
        else:
            copy(kind, d, False, lambda end: end.start())

    def carry_out(actions, lowest):
        transposed = False
        while actions:
            name, d = key = group(*actions[0])
            count = 1
            while count < len(actions) and group(*actions[count]) == key:
                count += 1
            batch, actions = actions[:count], actions[count:]

            def run(batch=batch):
                for action in batch:
                    act(*action, lowest)

            if not transposed and batch[0][0] != "start":
                zt[...] = gath[own].T
                transposed = True
            if lowest or d == 0:
                run()
            else:
                pl.when(z + d < planes)(run)

    pl.when(z == 0)(lambda: carry_out(plan(planes, True), True))
    if planes > 1:
        pl.when(z > 0)(lambda: carry_out(plan(planes, False), False))

    def finish(plane):
        counts = [0, 0]
        for action, kind, d in plan(planes, plane == 0):
            raw_sent = d == 0 and (kind == "ZA" or kind in STATS and plane < low)
            if action == "start" and plane + d < planes and not raw_sent:
                for c in range(2):
                    counts[c] += piece(kind, d, False, highs[c])[2][1]
        for c in range(2):
            pl.when(core == c)(lambda c=c: drain(counts[c], send.at[0]))
        raw_rows = (4 * (early_rows + stat_rows) if plane < low else 0) + (
            2 * (down_depth(bars) + stat_rows) if plane else 0
        )
        drain(raw_rows, send.at[1])
        part_wait(8 * low - (plane < low) + (planes - low if plane == low - 1 else 0)).wait_send()

    for plane in range(planes):
        pl.when(z == plane)(functools.partial(finish, plane))


def finish_kernel(early_ref, gath, zt, out_hbm, late_ref, sem):
    blocks, _, width = gath.shape
    own = lax.axis_index("blk") * 2 + lax.axis_index("grp")
    ready = width * (blocks - 8)
    copies = [pltpu.make_async_copy(early_ref, out_hbm.at[:, pl.ds(0, ready)], sem.at[0])]
    copies[0].start()
    for i in range(8):
        block = blocks - 8 + i
        product = jnp.dot(zt[...], gath[block], preferred_element_type=jnp.float32).astype(jnp.bfloat16)
        late_ref[:, width * i : width * (i + 1)] = jnp.where(block >= own, product, jnp.bfloat16(0.0))
        if i % 4 == 3:
            at = pl.ds(width * (i - 3), 4 * width)
            to = pl.ds(ready + width * (i - 3), 4 * width)
            copies.append(pltpu.make_async_copy(late_ref.at[:, at], out_hbm.at[:, to], sem.at[len(copies)]))
            copies[-1].start()
    for copy in copies:
        copy.wait()


def shards(planes, returns):
    bars, width = returns.shape
    blocks = planes * 8
    held = blocks * width * (2 * bars + 2 * width) + 6 * bars * width
    vmem = pl.BlockSpec(memory_space=pltpu.VMEM)
    products, gathered, transposed = pl.pallas_call(
        functools.partial(kernel, planes),
        out_shape=[
            jax.ShapeDtypeStruct((width, (blocks - 8) * width), jnp.bfloat16),
            jax.ShapeDtypeStruct((blocks, bars, width), jnp.bfloat16),
            jax.ShapeDtypeStruct((width, bars), jnp.bfloat16),
        ],
        in_specs=[pl.BlockSpec(memory_space=pltpu.HBM)],
        out_specs=[vmem, vmem, vmem],
        scratch_shapes=[
            pltpu.VMEM((bars, width), jnp.float32),
            pltpu.VMEM((blocks, 1, bars), jnp.float32),
            pltpu.VMEM((1, bars), jnp.float32),
            pltpu.VMEM((bars, 128), jnp.float32),
            pltpu.VMEM((3, max(early_depth(bars), down_depth(bars)), width), jnp.float32),
            pltpu.VMEM((4, width), jnp.float32),
            pltpu.VMEM((3, 4, width), jnp.float32),
            pltpu.SemaphoreType.DMA,
            pltpu.SemaphoreType.DMA,
            pltpu.SemaphoreType.DMA,
            pltpu.SemaphoreType.DMA((2,)),
            pltpu.SemaphoreType.DMA((14 * planes - 4,)),
        ],
        compiler_params=pltpu.CompilerParams(
            collective_id=0, has_side_effects=True, vmem_limit_bytes=held + 4 * 1024 * 1024
        ),
    )(pltpu.with_memory_space_constraint(returns, pltpu.HBM))
    return pl.pallas_call(
        finish_kernel,
        out_shape=jax.ShapeDtypeStruct((width, blocks * width), jnp.bfloat16),
        in_specs=[vmem, vmem, vmem],
        out_specs=pl.BlockSpec(memory_space=pltpu.HBM),
        scratch_shapes=[pltpu.VMEM((width, 8 * width), jnp.bfloat16), pltpu.SemaphoreType.DMA((3,))],
        compiler_params=pltpu.CompilerParams(vmem_limit_bytes=4 * 1024 * 1024),
    )(*(pltpu.with_memory_space_constraint(a, pltpu.VMEM) for a in (products, gathered, transposed)))


def solution(mesh):
    planes = mesh.shape["blk"] // 4
    in_specs = (P(None, ("blk", "grp")),)
    out_specs = P(("blk", "grp"), None)
    return jax.shard_map(
        functools.partial(shards, planes), mesh=mesh, in_specs=in_specs, out_specs=out_specs, check_vma=False
    )
```
